32 devices in a mesh: dp: 1 (over z), vp: 32 (over y, x, core).
Axes of the slice: x: 4, y: 4, z: 1, core: 2. Of those that a mesh axis runs over, the one named last changes fastest.
The devices are a block of a 4x4x8 slice.
Arguments:
- hidden: bfloat16 [256, 32, 2048], P('vp', 'dp')
- norm_gain: float32 [2048], replicated
- norm_bias: float32 [2048], replicated
- w_out: bfloat16 [2048, 49152], P(None, 'vp')
- labels: int32 [256, 32], P('vp', 'dp')
- loss_mask: float32 [256, 32], P('vp', 'dp')
Outputs:
- output 1: float32 [1], P('dp')
- output 2: bfloat16 [256, 32, 2048], P('vp', 'dp')
- output 3: float32 [2048, 49152], P('dp', 'vp')
- output 4: float32 [2048], P('dp')
- output 5: float32 [2048], P('dp')
All inputs are finite; a program needn't handle non-finite values.
Results may differ from the reference program's by a relative error of at most 0.001.
Values are sent between devices in bfloat16 or wider.
A program may use at most 768 MiB of HBM per device.

```python
import jax
import jax.numpy as jnp
from jax import lax

SEQ_DEV = 8
GROUP_SIZE = 32
BATCH_PART = 32
D_MODEL = 2048
VOCAB_SIZE = 49152
VOCAB_PAD = 49152
NORM_EPS = 1e-5
SEQ_LEN = SEQ_DEV * GROUP_SIZE
BLOCK_TOKENS = SEQ_DEV * BATCH_PART


def draw_labels(rng_key):
    key_pick, key_flat, key_upper, key_inner, key_skew = jax.random.split(rng_key, 5)
    tok_shape = (SEQ_LEN, BATCH_PART)
    flat_ids = jax.random.randint(key_flat, tok_shape, 0, VOCAB_SIZE)
    upper_one = jax.random.randint(key_upper, tok_shape, 1, VOCAB_SIZE + 1)
    upper_two = jax.random.randint(key_inner, tok_shape, 1, upper_one + 1)
    skew_ids = jax.random.randint(key_skew, tok_shape, 0, upper_two)
    pick_flat = jax.random.randint(key_pick, tok_shape, 0, 2)
    label_ids = jnp.where(pick_flat == 0, flat_ids, skew_ids)
    label_ids = label_ids.at[0, 0].set(VOCAB_SIZE - 1)
    return label_ids.at[SEQ_LEN - 1, BATCH_PART - 1].set(0)


def draw_mask(rng_key):
    mask_ids = jax.random.randint(rng_key, (SEQ_LEN, BATCH_PART), 0, 4)
    return (mask_ids > 0).astype(jnp.float32).at[0, 0].set(1.0)


def setup_inputs(seed: int = 0, part: int = 0) -> dict:
    root_key = jax.random.key(seed)
    shared_key, part_base = jax.random.split(root_key)
    part_key = jax.random.fold_in(part_base, part)
    key_w, key_g, key_c = jax.random.split(shared_key, 3)
    key_x, key_lab, key_mask = jax.random.split(part_key, 3)
    hidden = jax.random.normal(key_x, (SEQ_LEN, BATCH_PART, D_MODEL), jnp.float32).astype(jnp.bfloat16)
    norm_gain = 0.3 * jax.random.normal(key_g, (D_MODEL,), jnp.float32)
    norm_bias = 0.5 * jax.random.normal(key_c, (D_MODEL,), jnp.float32)
    w_out = (jax.random.normal(key_w, (D_MODEL, VOCAB_PAD), jnp.float32) * (2.0 / D_MODEL ** 0.5)).astype(jnp.bfloat16)
    labels = draw_labels(key_lab)
    loss_mask = draw_mask(key_mask)
    return {"hidden": hidden, "norm_gain": norm_gain, "norm_bias": norm_bias, "w_out": w_out, "labels": labels, "loss_mask": loss_mask}


def reference(hidden, norm_gain, norm_bias, w_out, labels, loss_mask):
    mask_total = jnp.sum(loss_mask)
    x_blocks = hidden.reshape(GROUP_SIZE, BLOCK_TOKENS, D_MODEL)
    lab_blocks = labels.reshape(GROUP_SIZE, BLOCK_TOKENS)
    mask_blocks = loss_mask.reshape(GROUP_SIZE, BLOCK_TOKENS)
    col_ids = jnp.arange(VOCAB_PAD, dtype=jnp.int32)

    def block_step(acc_state, block_in):
        grad_w, loss_sum, gain_sum, bias_sum = acc_state
        x_blk, lab_blk, mask_blk = block_in
        x_float = x_blk.astype(jnp.float32)
        tok_mean = jnp.mean(x_float, axis=-1, keepdims=True)
        centered = x_float - tok_mean
        inv_std = lax.rsqrt(jnp.mean(centered * centered, axis=-1, keepdims=True) + NORM_EPS)
        normed = centered * inv_std
        h_blk = (normed * (1.0 + norm_gain) + norm_bias).astype(jnp.bfloat16)
        logits = jnp.dot(h_blk, w_out, preferred_element_type=jnp.float32)
        row_max = jnp.max(logits, axis=-1, keepdims=True)
        exp_shift = jnp.exp(logits - row_max)
        sum_exp = jnp.sum(exp_shift, axis=-1, keepdims=True)
        is_label = (col_ids[None, :] == lab_blk[:, None]).astype(jnp.float32)
        target = jnp.sum(logits * is_label, axis=-1)
        tok_loss = row_max[:, 0] + jnp.log(sum_exp[:, 0]) - target
        tok_weight = mask_blk / mask_total
        grad_logits = ((exp_shift / sum_exp - is_label) * tok_weight[:, None]).astype(jnp.bfloat16)
        grad_w = grad_w + jnp.dot(h_blk.T, grad_logits, preferred_element_type=jnp.float32)
        grad_h = jnp.dot(grad_logits, w_out.T, preferred_element_type=jnp.float32)
        gain_sum = gain_sum + jnp.sum(grad_h * normed, axis=0)
        bias_sum = bias_sum + jnp.sum(grad_h, axis=0)
        scaled = grad_h * (1.0 + norm_gain)
        grad_x = inv_std * (scaled - jnp.mean(scaled, axis=-1, keepdims=True) - normed * jnp.mean(scaled * normed, axis=-1, keepdims=True))
        loss_sum = loss_sum + jnp.sum(mask_blk * tok_loss)
        return (grad_w, loss_sum, gain_sum, bias_sum), grad_x.astype(jnp.bfloat16)

    init_state = (jnp.zeros((D_MODEL, VOCAB_PAD), jnp.float32), jnp.zeros((), jnp.float32), jnp.zeros((D_MODEL,), jnp.float32), jnp.zeros((D_MODEL,), jnp.float32))
    final_state, grad_x = lax.scan(block_step, init_state, (x_blocks, lab_blocks, mask_blocks))
    grad_w, loss_sum, gain_sum, bias_sum = final_state
    loss = (loss_sum / mask_total).reshape(1)
    return loss, grad_x.reshape(SEQ_LEN, BATCH_PART, D_MODEL), grad_w, gain_sum, bias_sum
```

```python
import functools
import math

import jax
import jax.numpy as jnp
from jax import lax
from jax.experimental import pallas as pl
from jax.experimental.pallas import tpu as pltpu
from jax.sharding import PartitionSpec as P

NORM_EPS = 1e-5
MESH = pl.DeviceIdType.MESH
VMEM_LIMIT = 66_000_000
F32 = jnp.float32
BF16 = jnp.bfloat16


class Rings:
    def __init__(self, n):
        self.n = n
        self.chips = n // 2
        self.side = math.isqrt(self.chips)
        assert self.side * self.side * 2 == n
        self.me = lax.axis_index("vp")
        self.core = lax.rem(self.me, 2)
        chip = lax.div(self.me, 2)
        x, y = lax.rem(chip, self.side), lax.div(chip, self.side)
        k = lax.rem(x + y, self.side)
        self.spot = (y * self.side + k, x * self.side + k)
        self.sibling = self.me + 1 - 2 * self.core
        step = 2 * self.core - 1
        self.s_next = [self.at(c, lax.rem(self.spot[c] + step + self.chips, self.chips), 1 - self.core) for c in range(2)]
        self.x_prev = [self.at(c, lax.rem(self.spot[c] + step + self.chips, self.chips), 1 - self.core) for c in range(2)]

    def at(self, cycle, spot, core):
        q, k = lax.div(spot, self.side), lax.rem(spot, self.side)
        a = lax.rem(k - q + self.side, self.side)
        chip = q * self.side + a if cycle == 0 else a * self.side + q
        return chip * 2 + core

    def owner(self, group, quarter):
        cycle = quarter % 2
        pos = 2 * self.spot[cycle] + self.core
        shift = self.n - group if quarter < 2 else group
        origin = lax.rem(pos + shift + self.n, self.n)
        return self.at(cycle, lax.div(origin, 2), lax.rem(origin, 2))

    def greet(self, wait=True):
        barrier = pltpu.get_barrier_semaphore()
        for other in (self.sibling, *self.s_next):
            pl.semaphore_signal(barrier, inc=1, device_id={"vp": other}, device_id_type=MESH)

    def greeted(self):
        pl.semaphore_wait(pltpu.get_barrier_semaphore(), 3)


def norm_rows(x_rows):
    x = x_rows.astype(F32)
    centered = x - jnp.mean(x, axis=-1, keepdims=True)
    inv_std = lax.rsqrt(jnp.mean(centered * centered, axis=-1, keepdims=True) + NORM_EPS)
    return centered * inv_std, inv_std


def gather_kernel(n, x_ref, gain_ref, bias_ref, w_hbm, h_hbm, z_hbm, lse_ref,
                  w_v, h_all, zbuf, col, w_sem, h_sem, z_sem, send_x, send_s, recv_x, recv_s):
    ring = Rings(n)
    rows, dim = x_ref.shape
    cols = w_v.shape[1]
    half, quart, piece, wide = rows // 2, rows // 4, rows // 8, cols // 2
    xo = pl.multiple_of(half * ring.core, half)
    so = pl.multiple_of(half * (1 - ring.core), half)

    w_copy = pltpu.make_async_copy(w_hbm, w_v, w_sem)
    w_copy.start()
    ring.greet()

    ln_rows = min(32, rows)

    @pl.loop(0, rows // ln_rows)
    def _(b):
        r = pl.ds(pl.multiple_of(b * ln_rows, ln_rows), ln_rows)
        normed, _ = norm_rows(x_ref[r, :])
        h_all[0, r, :] = (normed * (1.0 + gain_ref[...]) + bias_ref[...]).astype(BF16)

    ring.greeted()

    def x_copy(i, c, u):
        r = pl.ds(xo + (c * quart + u * piece), piece)
        return pltpu.make_async_remote_copy(
            src_ref=h_all.at[i, r], dst_ref=h_all.at[i + 1, r],
            send_sem=send_x.at[lax.rem(i, 4), c, u], recv_sem=recv_s.at[i + 1, c, u],
            device_id={"vp": ring.sibling}, device_id_type=MESH)

    def s_copy(i, c, u):
        r = pl.ds(so + (c * quart + u * piece), piece)
        return pltpu.make_async_remote_copy(
            src_ref=h_all.at[i, r], dst_ref=h_all.at[i + 1, r],
            send_sem=send_s.at[lax.rem(i, 4), c, u], recv_sem=recv_x.at[i + 1, c, u],
            device_id={"vp": ring.s_next[c]}, device_id_type=MESH)

    def x_arrived(i, c, u):
        r = pl.ds(xo + (c * quart + u * piece), piece)
        pltpu.make_async_remote_copy(
            src_ref=h_all.at[i, r], dst_ref=h_all.at[i, r],
            send_sem=send_s.at[0, c, u], recv_sem=recv_x.at[i, c, u],
            device_id={"vp": ring.s_next[c]}, device_id_type=MESH).wait_recv()

    def s_arrived(i, c, u):
        r = pl.ds(so + (c * quart + u * piece), piece)
        pltpu.make_async_remote_copy(
            src_ref=h_all.at[i, r], dst_ref=h_all.at[i, r],
            send_sem=send_x.at[0, c, u], recv_sem=recv_s.at[i, c, u],
            device_id={"vp": ring.sibling}, device_id_type=MESH).wait_recv()

    def send(copy, i, c, u):
        @pl.when(i >= 4)
        def _():
            copy(i - 4, c, u).wait_send()
        copy(i, c, u).start()

    def z_out(g):
        return pltpu.make_async_copy(zbuf.at[lax.rem(g, 2)], z_hbm.at[g], z_sem.at[lax.rem(g, 2)])

    def h_out(g):
        return pltpu.make_async_copy(h_all.at[g], h_hbm.at[g], h_sem.at[lax.rem(g, 2)])

    stat_rows = min(32, half)

    def stats(slot, u):
        for b in range(half // stat_rows):
            z = zbuf[slot, pl.ds(u * half + b * stat_rows, stat_rows), :]
            top = jnp.max(z, axis=-1, keepdims=True)
            lse = top + jnp.log(jnp.sum(jnp.exp(z - top), axis=-1, keepdims=True))
            col[pl.ds(b * stat_rows, stat_rows), :] = jnp.broadcast_to(lse, (stat_rows, col.shape[1]))
        return jnp.transpose(col[...])[0:1, :]

    def put(row, g, u):
        for c in range(2):
            q = 2 * u + c
            lse_ref[ring.owner(g, q), :, q * quart:(q + 1) * quart] = row[:, c * quart:(c + 1) * quart]

    def logits(g, u):
        part = slice(u * wide, (u + 1) * wide)
        zbuf[lax.rem(g, 2), :, part] = jnp.dot(h_all[g], w_v[:, part], preferred_element_type=F32)

    zbuf[...] = jnp.zeros_like(zbuf)
    for c in range(2):
        s_copy(0, c, 0).start()
    w_copy.wait()

    @pl.loop(0, n)
    def _(i):
        g = i - 1
        for u in range(2):
            @pl.when(i >= 1)
            def _():
                for c in range(2):
                    x_arrived(i, c, u)

            @pl.when(i < n - 1)
            def _():
                for c in range(2):
                    send(x_copy, i, c, u)

            j = i + u

            @pl.when((j >= 1) & (j < n))
            def _():
                for c in range(2):
                    s_arrived(j, c, 1 - u)

            @pl.when(j < n - 1)
            def _():
                for c in range(2):
                    send(s_copy, j, c, 1 - u)

            @pl.when(i >= 1)
            def _():
                if u == 0:
                    @pl.when(g >= 2)
                    def _():
                        z_out(g - 2).wait()
                        h_out(g - 2).wait()
                    h_out(g).start()
                logits(g, u)
                row = stats(lax.rem(g + 1, 2), u)
                put(row, lax.max(g - 1, 0), u)
                if u == 1:
                    z_out(g).start()

    last = n - 1
    z_out(last - 2).wait()
    h_out(last - 2).wait()
    h_out(last).start()
    for u in range(2):
        logits(last, u)
        put(stats(lax.rem(last + 1, 2), u), last - 1, u)
    z_out(last).start()
    for u in range(2):
        put(stats(last % 2, u), last, u)
    for g in (last - 1, last):
        z_out(g).wait()
        h_out(g).wait()
    for i in range(n - 5, n - 1):
        for c in range(2):
            for u in range(2):
                x_copy(i, c, u).wait_send()
                s_copy(i, c, u).wait_send()


def gather_logits(n, x, gain, bias, w):
    rows, dim = x.shape
    cols = w.shape[1]
    vmem = pl.BlockSpec(memory_space=pltpu.VMEM)
    hbm = pl.BlockSpec(memory_space=pl.ANY)
    return pl.pallas_call(
        functools.partial(gather_kernel, n),
        out_shape=(
            jax.ShapeDtypeStruct((n, rows, dim), BF16),
            jax.ShapeDtypeStruct((n, rows, cols), F32),
            jax.ShapeDtypeStruct((n, 1, rows), F32),
        ),
        in_specs=[vmem, vmem, vmem, hbm],
        out_specs=(hbm, hbm, vmem),
        scratch_shapes=[
            pltpu.VMEM((dim, cols), BF16),
            pltpu.VMEM((n, rows, dim), BF16),
            pltpu.VMEM((2, rows, cols), F32),
            pltpu.VMEM((rows // 2, 128), F32),
            pltpu.SemaphoreType.DMA,
            pltpu.SemaphoreType.DMA((2,)),
            pltpu.SemaphoreType.DMA((2,)),
            pltpu.SemaphoreType.DMA((4, 2, 2)),
            pltpu.SemaphoreType.DMA((4, 2, 2)),
            pltpu.SemaphoreType.DMA((n, 2, 2)),
            pltpu.SemaphoreType.DMA((n, 2, 2)),
        ],
        compiler_params=pltpu.CompilerParams(collective_id=0, has_side_effects=True, vmem_limit_bytes=VMEM_LIMIT),
        name="gather_logits",
    )(x, gain.reshape(1, dim), bias.reshape(1, dim), w)


def greet_all(n, me):
    barrier = pltpu.get_barrier_semaphore()
    for d in range(1, n):
        pl.semaphore_signal(barrier, inc=1, device_id={"vp": lax.rem(me + d, n)}, device_id_type=MESH)
    pl.semaphore_wait(barrier, n - 1)


def stats_kernel(n, mine_ref, tok_ref, lse_ref, toks_ref, got, total, send_a, recv_a, send_b, recv_b, send_c, recv_c):
    me = lax.axis_index("vp")
    greet_all(n, me)

    def hop(src, dst, send_sem, recv_sem, d):
        return pltpu.make_async_remote_copy(
            src_ref=src, dst_ref=dst, send_sem=send_sem.at[d], recv_sem=recv_sem.at[d],
            device_id={"vp": lax.rem(me + d, n)}, device_id_type=MESH)

    def first(d):
        return hop(mine_ref.at[lax.rem(me + d, n)], got.at[d], send_a, recv_a, d)

    def toks(d):
        return hop(tok_ref, toks_ref.at[me], send_b, recv_b, d)

    def second(d):
        return hop(total, lse_ref.at[me], send_c, recv_c, d)

    @pl.loop(1, n)
    def _(d):
        first(d).start()

    @pl.loop(1, n)
    def _(d):
        toks(d).start()

    got[0] = mine_ref[me]
    toks_ref[me] = tok_ref[...]

    @pl.loop(1, n)
    def _(d):
        first(d).wait_recv()

    parts = got[...]
    top = jnp.max(parts, axis=0)
    lse = top + jnp.log(jnp.sum(jnp.exp(parts - top[None]), axis=0))
    total[...] = lse
    lse_ref[me] = lse

    @pl.loop(1, n)
    def _(d):
        second(d).start()

    @pl.loop(1, n)
    def _(d):
        second(d).wait()
        toks(d).wait()
        first(d).wait_send()


def token_stats(n, mine, toks):
    rows = mine.shape[-1]
    vmem = pl.BlockSpec(memory_space=pltpu.VMEM)
    return pl.pallas_call(
        functools.partial(stats_kernel, n),
        out_shape=(jax.ShapeDtypeStruct((n, 1, rows), F32), jax.ShapeDtypeStruct((n, 1, 2 * rows), F32)),
        in_specs=[vmem, vmem],
        out_specs=(vmem, vmem),
        scratch_shapes=[pltpu.VMEM((n, 1, rows), F32), pltpu.VMEM((1, rows), F32)]
        + [pltpu.SemaphoreType.DMA((n,))] * 6,
        compiler_params=pltpu.CompilerParams(collective_id=1, has_side_effects=True),
        name="token_stats",
    )(mine, toks)


SLOTS = 8
LAG = 2
PIECES = 4


def scatter_kernel(n, z_hbm, h_hbm, w_hbm, lse_ref, toks_ref, dw_hbm, dh_ref, t_ref,
                   w_v, dw, zb, hb, dzb, part, from_x, from_s, flat, cols, total, w_sem, z_sem, h_sem, dw_sem,
                   send_x, send_s, recv_x, recv_s, credit_x, credit_s):
    ring = Rings(n)
    rows, dim = dh_ref.shape
    vocab = w_v.shape[1]
    half, quart, wide = rows // 2, rows // 4, dim // PIECES
    xo = pl.multiple_of(half * ring.core, half)
    so = pl.multiple_of(half * (1 - ring.core), half)
    col_start = ring.me * vocab

    w_copy = pltpu.make_async_copy(w_hbm, w_v, w_sem)
    w_copy.start()
    ring.greet()

    def fetch(hbm, buf, sem, j):
        slot = lax.rem(j, 2)
        return [
            pltpu.make_async_copy(
                hbm.at[lax.rem(j + ahead, n), pl.ds(off, half)], buf.at[slot, pl.ds(off, half)], sem.at[slot, ahead])
            for ahead, off in ((0, xo), (1, so))
        ]

    for copy in fetch(z_hbm, zb, z_sem, 0) + fetch(h_hbm, hb, h_sem, 0) + fetch(z_hbm, zb, z_sem, 1):
        copy.start()

    mask_total = jnp.sum(jnp.sum(toks_ref[:, :, rows:], axis=0), axis=-1, keepdims=True)
    total[...] = jnp.zeros_like(total)
    flat[...] = jnp.zeros_like(flat)
    t_ref[...] = jnp.zeros_like(t_ref)
    dw[...] = jnp.zeros_like(dw)

    def columns(j):
        for q in range(4):
            is_x = ring.core == q // 2
            group = lax.rem(jnp.where(is_x, j, j + 1), n)
            valid = jnp.where(is_x, jnp.where((j >= 1) & (j <= n), 1.0, 0.0), jnp.where(j < n, 1.0, 0.0))
            who = ring.owner(group, q)
            lanes = slice(q * quart, (q + 1) * quart)
            flat[0:1, lanes] = toks_ref[who][:, lanes] - col_start.astype(F32)
            flat[1:2, lanes] = toks_ref[who][:, rows + q * quart:rows + (q + 1) * quart] * valid / mask_total
            flat[2:3, lanes] = lse_ref[who][:, lanes]
        cols[...] = jnp.transpose(flat[...])

    dz_rows = min(16, quart)

    def make_dz(j, u):
        slot = lax.rem(j, 2)
        for b in range(rows // PIECES // dz_rows):
            r = pl.ds(u * (rows // PIECES) + b * dz_rows, dz_rows)
            z = zb[slot, r, :]
            label = cols[r, 0:1].astype(jnp.int32)
            weight = cols[r, 1:2]
            prob = jnp.exp(z - cols[r, 2:3])
            hit = lax.broadcasted_iota(jnp.int32, z.shape, 1) == label
            dzb[slot, r, :] = (jnp.where(hit, prob - 1.0, prob) * weight).astype(BF16)
            taken = jnp.where(hit, z * weight, 0.0)
            acc = taken[:, 0:128]
            for v in range(1, vocab // 128):
                acc = acc + taken[:, v * 128:(v + 1) * 128]
            t_ref[...] += acc

    def matmuls(j, u, slot):
        dz = dzb[lax.rem(j, 2)]
        d = slice(u * wide, (u + 1) * wide)
        part[slot] = lax.dot_general(dz, w_v[d, :], (((1,), (1,)), ((), ())), preferred_element_type=F32)
        dw[d, :] += lax.dot_general(hb[lax.rem(j, 2), :, d], dz, (((0,), (0,)), ((), ())), preferred_element_type=F32)

    def x_copy(k, c):
        slot = lax.rem(k, SLOTS)
        return pltpu.make_async_remote_copy(
            src_ref=part.at[slot, pl.ds(xo + c * quart, quart)], dst_ref=from_s.at[slot, c],
            send_sem=send_x.at[slot, c], recv_sem=recv_s.at[slot, c],
            device_id={"vp": ring.sibling}, device_id_type=MESH)

    def s_copy(k, c):
        slot = lax.rem(k, SLOTS)
        return pltpu.make_async_remote_copy(
            src_ref=part.at[slot, pl.ds(so + c * quart, quart)], dst_ref=from_x.at[slot, c],
            send_sem=send_s.at[slot, c], recv_sem=recv_x.at[slot, c],
            device_id={"vp": ring.s_next[c]}, device_id_type=MESH)

    def x_arrived(k, c):
        s_copy(k, c).wait_recv()

    def s_arrived(k, c):
        x_copy(k, c).wait_recv()

    x_lo, x_hi = PIECES, PIECES * n
    s_hi = PIECES * (n - 1)

    def do_x(j, u, k, slot):
        @pl.when(k >= SLOTS)
        def _():
            for c in range(2):
                x_arrived(k, c)
                r = pl.ds(xo + c * quart, quart)
                part[slot, r, :] += from_x[slot, c]

                @pl.when(k < s_hi)
                def _():
                    pl.semaphore_signal(credit_s.at[c], inc=1, device_id={"vp": ring.x_prev[c]}, device_id_type=MESH)

        @pl.when((k >= x_lo) & (k < x_hi))
        def _():
            for c in range(2):
                @pl.when(k >= x_lo + SLOTS)
                def _():
                    pl.semaphore_wait(credit_x.at[c], 1)
                x_copy(k, c).start()

        @pl.when(j == n)
        def _():
            dh_ref[pl.ds(xo, half), u * wide:(u + 1) * wide] = part[slot, pl.ds(xo, half), :]

    def do_s(j, u, k, slot):
        @pl.when((k >= x_lo) & (k < x_hi))
        def _():
            for c in range(2):
                s_arrived(k, c)
                r = pl.ds(so + c * quart, quart)
                part[slot, r, :] += from_s[slot, c]

                @pl.when(k < x_hi - SLOTS)
                def _():
                    pl.semaphore_signal(credit_x.at[c], inc=1, device_id={"vp": ring.sibling}, device_id_type=MESH)

        @pl.when((k >= 0) & (k < s_hi))
        def _():
            for c in range(2):
                @pl.when(k >= SLOTS)
                def _():
                    pl.semaphore_wait(credit_s.at[c], 1)
                s_copy(k, c).start()

        @pl.when(j == n - 1)
        def _():
            dh_ref[pl.ds(so, half), u * wide:(u + 1) * wide] = part[slot, pl.ds(so, half), :]

    for copy in fetch(z_hbm, zb, z_sem, 0):
        copy.wait()
    columns(0)
    for u in range(PIECES):
        make_dz(0, u)
    for copy in fetch(h_hbm, hb, h_sem, 0):
        copy.wait()
    w_copy.wait()
    ring.greeted()

    @pl.loop(0, n + 1)
    def _(j):
        @pl.when(j < n)
        def _():
            for copy in fetch(z_hbm, zb, z_sem, j + 1):
                copy.wait()
            for copy in fetch(h_hbm, hb, h_sem, j + 1):
                copy.start()

        @pl.when(j < n - 1)
        def _():
            for copy in fetch(z_hbm, zb, z_sem, j + 2):
                copy.start()

        columns(j + 1)
        for u in range(PIECES):
            k = PIECES * j + u
            slot = lax.rem(k, SLOTS)

            @pl.when((k >= SLOTS + x_lo))
            def _():
                for c in range(2):
                    x_copy(k - SLOTS, c).wait_send()

            @pl.when((k >= SLOTS) & (k < s_hi + SLOTS))
            def _():
                for c in range(2):
                    s_copy(k - SLOTS, c).wait_send()

            matmuls(j, u, slot)
            make_dz(j + 1, u)
            do_x(j, u, k, slot)
            ks = k - LAG
            js = j if u >= LAG else j - 1
            do_s(js, (u - LAG) % PIECES, ks, lax.rem(ks + SLOTS, SLOTS))

        @pl.when(j < n)
        def _():
            for copy in fetch(h_hbm, hb, h_sem, j + 1):
                copy.wait()

    dw_out = pltpu.make_async_copy(dw, dw_hbm, dw_sem)
    dw_out.start()
    for u in range(PIECES):
        for c in range(2):
            x_copy(x_hi - PIECES + u, c).wait_send()
    dw_out.wait()


def scatter_grads(n, z, h, w, lse, toks):
    _, rows, vocab = z.shape
    dim = w.shape[0]
    vmem = pl.BlockSpec(memory_space=pltpu.VMEM)
    hbm = pl.BlockSpec(memory_space=pl.ANY)
    wide = dim // PIECES
    return pl.pallas_call(
        functools.partial(scatter_kernel, n),
        out_shape=(
            jax.ShapeDtypeStruct((dim, vocab), F32),
            jax.ShapeDtypeStruct((rows, dim), F32),
            jax.ShapeDtypeStruct((16, 128), F32),
        ),
        in_specs=[hbm, hbm, hbm, vmem, vmem],
        out_specs=(hbm, vmem, vmem),
        scratch_shapes=[
            pltpu.VMEM((dim, vocab), BF16),
            pltpu.VMEM((dim, vocab), F32),
            pltpu.VMEM((2, rows, vocab), F32),
            pltpu.VMEM((2, rows, dim), BF16),
            pltpu.VMEM((2, rows, vocab), BF16),
            pltpu.VMEM((SLOTS, rows, wide), F32),
            pltpu.VMEM((SLOTS, 2, rows // 4, wide), F32),
            pltpu.VMEM((SLOTS, 2, rows // 4, wide), F32),
            pltpu.VMEM((128, rows), F32),
            pltpu.VMEM((rows, 128), F32),
            pltpu.VMEM((8, 128), F32),
            pltpu.SemaphoreType.DMA,
            pltpu.SemaphoreType.DMA((2, 2)),
            pltpu.SemaphoreType.DMA((2, 2)),
            pltpu.SemaphoreType.DMA,
            pltpu.SemaphoreType.DMA((SLOTS, 2)),
            pltpu.SemaphoreType.DMA((SLOTS, 2)),
            pltpu.SemaphoreType.DMA((SLOTS, 2)),
            pltpu.SemaphoreType.DMA((SLOTS, 2)),
            pltpu.SemaphoreType.REGULAR((2,)),
            pltpu.SemaphoreType.REGULAR((2,)),
        ],
        compiler_params=pltpu.CompilerParams(collective_id=2, has_side_effects=True, vmem_limit_bytes=VMEM_LIMIT),
        name="scatter_grads",
    )(z, h, w, lse, toks)


def finish_kernel(n, dh_ref, x_ref, gain_ref, t_ref, lse_ref, toks_ref, dx_ref, sums_ref, loss_ref, mine, got, send_sem, recv_sem):
    me = lax.axis_index("vp")
    rows, dim = dh_ref.shape
    blk = min(16, rows)
    barrier = pltpu.get_barrier_semaphore()
    for d in range(1, n):
        pl.semaphore_signal(barrier, inc=1, device_id={"vp": lax.rem(me + d, n)}, device_id_type=MESH)

    def body(b, carry):
        dg, dc = carry
        r = pl.ds(pl.multiple_of(b * blk, blk), blk)
        normed, inv_std = norm_rows(x_ref[r, :])
        dh = dh_ref[r, :]
        dg = dg + jnp.sum(dh * normed, axis=0, keepdims=True)
        dc = dc + jnp.sum(dh, axis=0, keepdims=True)
        scaled = dh * (1.0 + gain_ref[...])
        mean_s = jnp.mean(scaled, axis=-1, keepdims=True)
        mean_sn = jnp.mean(scaled * normed, axis=-1, keepdims=True)
        dx_ref[r, :] = (inv_std * (scaled - mean_s - normed * mean_sn)).astype(BF16)
        return dg, dc

    zero = jnp.zeros((1, dim), F32)
    dg, dc = lax.fori_loop(0, rows // blk, body, (zero, zero))
    mine[:, 0:dim] = dg
    mine[:, dim:2 * dim] = dc
    mine[:, 2 * dim:] = jnp.sum(t_ref[...], axis=0, keepdims=True)
    pl.semaphore_wait(barrier, n - 1)

    def hop(d):
        return pltpu.make_async_remote_copy(
            src_ref=mine, dst_ref=got.at[me], send_sem=send_sem.at[d], recv_sem=recv_sem.at[d],
            device_id={"vp": lax.rem(me + d, n)}, device_id_type=MESH)

    @pl.loop(1, n)
    def _(d):
        hop(d).start()

    got[me] = mine[...]
    mask = toks_ref[:, :, rows:]
    mask_total = jnp.sum(jnp.sum(mask, axis=0), axis=-1, keepdims=True)
    lse_sum = jnp.sum(jnp.sum(lse_ref[...] * (mask / mask_total[None]), axis=0), axis=-1, keepdims=True)

    @pl.loop(1, n)
    def _(d):
        hop(d).wait()

    sums = jnp.sum(got[...], axis=0)
    sums_ref[...] = sums[:, :2 * dim]
    loss_ref[...] = jnp.broadcast_to(lse_sum - jnp.sum(sums[:, 2 * dim:], axis=-1, keepdims=True), loss_ref.shape)


def finish(n, dh, x, gain, t, lse, toks):
    rows, dim = dh.shape
    vmem = pl.BlockSpec(memory_space=pltpu.VMEM)
    return pl.pallas_call(
        functools.partial(finish_kernel, n),
        out_shape=(
            jax.ShapeDtypeStruct((rows, dim), BF16),
            jax.ShapeDtypeStruct((1, 2 * dim), F32),
            jax.ShapeDtypeStruct((1, 128), F32),
        ),
        in_specs=[vmem] * 6,
        out_specs=(vmem, vmem, vmem),
        scratch_shapes=[
            pltpu.VMEM((1, 2 * dim + 128), F32),
            pltpu.VMEM((n, 1, 2 * dim + 128), F32),
            pltpu.SemaphoreType.DMA((n,)),
            pltpu.SemaphoreType.DMA((n,)),
        ],
        compiler_params=pltpu.CompilerParams(collective_id=3, has_side_effects=True),
        name="finish",
    )(dh, x, gain.reshape(1, dim), t, lse, toks)


def solution(mesh):
    n = mesh.shape["vp"]

    def per_device(hidden, norm_gain, norm_bias, w_blk, labels, loss_mask):
        dim = hidden.shape[-1]
        x = hidden.reshape(-1, dim)
        rows = x.shape[0]
        h, z, mine = gather_logits(n, x, norm_gain, norm_bias, w_blk)
        toks_mine = jnp.concatenate([labels.reshape(1, rows).astype(F32), loss_mask.reshape(1, rows)], axis=1)
        lse, toks = token_stats(n, mine, toks_mine)
        grad_w, dh, t = scatter_grads(n, z, h, w_blk, lse, toks)
        grad_x, sums, loss = finish(n, dh, x, norm_gain, t, lse, toks)
        return loss[0, :1], grad_x.reshape(hidden.shape), grad_w, sums[0, :dim], sums[0, dim:]

    tok_spec = P("vp", "dp")
    return jax.shard_map(
        per_device,
        mesh=mesh,
        in_specs=(P("vp", "dp", None), P(None), P(None), P(None, "vp"), tok_spec, tok_spec),
        out_specs=(P("dp"), P("vp", "dp", None), P("dp", "vp"), P("dp"), P("dp")),
        check_vma=False,
    )
```

```python
import functools
import math

import jax
import jax.numpy as jnp
from jax import lax
from jax.experimental import pallas as pl
from jax.experimental.pallas import tpu as pltpu
from jax.sharding import PartitionSpec as P

NORM_EPS = 1e-5
MESH = pl.DeviceIdType.MESH
GATHER_VMEM = 62_000_000
F32 = jnp.float32
BF16 = jnp.bfloat16


class Rings:
    def __init__(self, n):
        self.n = n
        self.chips = n // 2
        self.side = math.isqrt(self.chips)
        assert self.side * self.side * 2 == n
        self.me = lax.axis_index("vp")
        self.core = lax.rem(self.me, 2)
        chip = lax.div(self.me, 2)
        x, y = lax.rem(chip, self.side), lax.div(chip, self.side)
        k = lax.rem(x + y, self.side)
        self.spot = (y * self.side + k, x * self.side + k)
        self.sibling = self.me + 1 - 2 * self.core
        step = 2 * self.core - 1
        self.s_next = [self.at(c, lax.rem(self.spot[c] + step + self.chips, self.chips), 1 - self.core) for c in range(2)]
        self.x_prev = [self.at(c, lax.rem(self.spot[c] + step + self.chips, self.chips), 1 - self.core) for c in range(2)]

    def at(self, cycle, spot, core):
        q, k = lax.div(spot, self.side), lax.rem(spot, self.side)
        a = lax.rem(k - q + self.side, self.side)
        chip = q * self.side + a if cycle == 0 else a * self.side + q
        return chip * 2 + core

    def owner(self, group, quarter):
        cycle = quarter % 2
        pos = 2 * self.spot[cycle] + self.core
        shift = self.n - group if quarter < 2 else group
        origin = lax.rem(pos + shift + self.n, self.n)
        return self.at(cycle, lax.div(origin, 2), lax.rem(origin, 2))

    def greet(self):
        barrier = pltpu.get_barrier_semaphore()
        for other in (self.sibling, *self.s_next):
            pl.semaphore_signal(barrier, inc=1, device_id={"vp": other}, device_id_type=MESH)

    def greeted(self):
        pl.semaphore_wait(pltpu.get_barrier_semaphore(), 3)


def norm_rows(x_rows):
    x = x_rows.astype(F32)
    centered = x - jnp.mean(x, axis=-1, keepdims=True)
    inv_std = lax.rsqrt(jnp.mean(centered * centered, axis=-1, keepdims=True) + NORM_EPS)
    return centered * inv_std, inv_std


def signal_all(n, me):
    barrier = pltpu.get_barrier_semaphore()
    for d in range(1, n):
        pl.semaphore_signal(barrier, inc=1, device_id={"vp": lax.rem(me + d, n)}, device_id_type=MESH)


def gather_kernel(n, x_ref, gain_ref, bias_ref, tok_ref, w_hbm, h_hbm, z_hbm, wt_hbm, lse_ref, toks_ref,
                  w_v, wt_v, h_all, zbuf, col, local, got, own, w_sem, wt_sem, h_sem, z_sem, send_x, send_s, send_d, recv_x, recv_s,
                  stat_send, stat_recv, lse_send, lse_recv, tok_send, tok_recv):
    ring = Rings(n)
    me = ring.me
    rows, dim = x_ref.shape
    cols = w_v.shape[1]
    half, quart, piece, wide = rows // 2, rows // 4, rows // 8, cols // 2
    xo = pl.multiple_of(half * ring.core, half)
    so = pl.multiple_of(half * (1 - ring.core), half)

    w_copy = pltpu.make_async_copy(w_hbm, w_v, w_sem)
    w_copy.start()
    signal_all(n, me)

    ln_rows = min(64, rows)

    @pl.loop(0, rows // ln_rows)
    def _(b):
        r = pl.ds(pl.multiple_of(b * ln_rows, ln_rows), ln_rows)
        normed, _ = norm_rows(x_ref[r, :])
        h_all[0, r, :] = (normed * (1.0 + gain_ref[...]) + bias_ref[...]).astype(BF16)

    pl.semaphore_wait(pltpu.get_barrier_semaphore(), n - 1)

    def hop(src, dst, send_sem, recv_sem, who):
        return pltpu.make_async_remote_copy(
            src_ref=src, dst_ref=dst, send_sem=send_sem, recv_sem=recv_sem,
            device_id={"vp": who}, device_id_type=MESH)

    def x_copy(i, c, u):
        r = pl.ds(xo + (c * quart + u * piece), piece)
        return hop(h_all.at[i, r], h_all.at[i + 1, r], send_x.at[lax.rem(i, 4), c, u], recv_s.at[i + 1, c, u], ring.sibling)

    def s_copy(i, c, u):
        r = pl.ds(so + (c * quart + u * piece), piece)
        return hop(h_all.at[i, r], h_all.at[i + 1, r], send_s.at[lax.rem(i, 4), c, u], recv_x.at[i + 1, c, u], ring.s_next[c])

    def d_copy(c, u):
        r = pl.ds(so + (c * quart + u * piece), piece)
        return hop(h_all.at[0, r], h_all.at[n - 1, r], send_d.at[c, u], recv_x.at[n - 1, c, u], ring.sibling)

    def x_arrived(i, c, u):
        r = pl.ds(xo + (c * quart + u * piece), piece)
        hop(h_all.at[i, r], h_all.at[i, r], send_s.at[0, c, u], recv_x.at[i, c, u], ring.s_next[c]).wait_recv()

    def s_arrived(i, c, u):
        r = pl.ds(so + (c * quart + u * piece), piece)
        hop(h_all.at[i, r], h_all.at[i, r], send_x.at[0, c, u], recv_s.at[i, c, u], ring.sibling).wait_recv()

    def send(copy, i, c, u):
        @pl.when(i >= 4)
        def _():
            copy(i - 4, c, u).wait_send()
        copy(i, c, u).start()

    def z_out(g, slot):
        return pltpu.make_async_copy(zbuf.at[slot], z_hbm.at[g], z_sem.at[slot])

    def h_out(g, slot):
        return pltpu.make_async_copy(h_all.at[g], h_hbm.at[g], h_sem.at[slot])

    stat_rows = min(32, half)

    def stats(slot, u):
        for b in range(half // stat_rows):
            z = zbuf[slot, u * half + b * stat_rows:u * half + (b + 1) * stat_rows, :]
            top = jnp.max(z, axis=-1, keepdims=True)
            lse = top + jnp.log(jnp.sum(jnp.exp(z - top), axis=-1, keepdims=True))
            col[b * stat_rows:(b + 1) * stat_rows, :] = jnp.broadcast_to(lse, (stat_rows, col.shape[1]))
        return jnp.transpose(col[...])[0:1, :]

    def stat_copy(g, u, c):
        q = 2 * u + c
        return hop(local.at[g, u], got.at[g, q], stat_send, stat_recv, ring.owner(g, q))

    def send_stats(g):
        for u in range(2):
            for c in range(2):
                stat_copy(g, u, c).start()

    def logits(g, slot, u):
        part = slice(u * wide, (u + 1) * wide)
        zbuf[slot, :, part] = jnp.dot(h_all[g], w_v[:, part], preferred_element_type=F32)

    strip = dim // n

    def flip(a, b):
        r = pl.ds(pl.multiple_of(a * (2 * strip), 2 * strip), 2 * strip)
        part = slice(b * wide, (b + 1) * wide)
        wt_v[part, r] = jnp.transpose(w_v[r, part])

    def tok_copy(d):
        return hop(tok_ref, toks_ref.at[me], tok_send, tok_recv, lax.rem(me + d, n))

    def lse_copy(d):
        return hop(own, lse_ref.at[me], lse_send, lse_recv, lax.rem(me + d, n))

    for c in range(2):
        s_copy(0, c, 0).start()
    zbuf[...] = jnp.zeros_like(zbuf)
    w_copy.wait()

    @pl.loop(0, n // 2)
    def _(a):
        for b in range(2):
            i = 2 * a + b
            for u in range(2):
                @pl.when(i >= 1)
                def _():
                    for c in range(2):
                        x_arrived(i, c, u)

                @pl.when(i < n - 1)
                def _():
                    for c in range(2):
                        send(x_copy, i, c, u)

                j = i + u

                @pl.when((j >= 1) & (j < n))
                def _():
                    for c in range(2):
                        s_arrived(j, c, 1 - u)

                @pl.when(j < n - 2)
                def _():
                    for c in range(2):
                        send(s_copy, j, c, 1 - u)

                if u == 0:
                    flip(a, b)
                else:
                    @pl.when(i == 0)
                    def _():
                        for c in range(2):
                            for v in range(2):
                                d_copy(c, v).start()

                        @pl.loop(1, n)
                        def _(d):
                            tok_copy(d).start()

                    @pl.when(i >= 3)
                    def _():
                        send_stats(i - 2)

                if u == 0:
                    @pl.when(i >= 1)
                    def _():
                        logits(i - 1, 1 - b, 1)
                        local[lax.max(i - 2, 0), 1] = stats(b, 1)
                        z_out(i - 1, 1 - b).start()
                else:
                    @pl.when(i >= 2)
                    def _():
                        z_out(i - 2, b).wait()
                        h_out(i - 2, b).wait()
                    h_out(i, b).start()
                    logits(i, b, 0)
                    local[lax.max(i - 1, 0), 0] = stats(1 - b, 0)

    last = n - 1
    wt_copy = pltpu.make_async_copy(wt_v, wt_hbm, wt_sem)
    wt_copy.start()
    logits(last, 1, 1)
    local[last - 1, 1] = stats(0, 1)
    z_out(last, 1).start()
    for u in range(2):
        local[last, u] = stats(1, u)
    send_stats(last - 1)
    send_stats(last)
    for q in range(4):
        got[0, q] = local[0, q // 2]
    toks_ref[me] = tok_ref[...]

    everyone = pl.ds(1, n - 1)
    stats_total = hop(got.at[everyone], got.at[everyone], stat_send, stat_recv, ring.sibling)
    stats_total.wait_recv()
    for q in range(4):
        parts = got[:, q]
        top = jnp.max(parts, axis=0)
        lse = top + jnp.log(jnp.sum(jnp.exp(parts - top[None]), axis=0))
        lanes = slice((q % 2) * quart, (q % 2 + 1) * quart)
        own[:, q * quart:(q + 1) * quart] = lse[:, lanes]
    lse_ref[me] = own[...]

    @pl.loop(1, n)
    def _(d):
        lse_copy(d).start()

    for c in range(2):
        for u in range(2):
            d_copy(c, u).wait_send()
            for i in range(n - 5, n - 1):
                x_copy(i, c, u).wait_send()
            for i in range(n - 6, n - 2):
                s_copy(i, c, u).wait_send()
    stats_total.wait_send()
    toks_total = hop(toks_ref.at[everyone], toks_ref.at[everyone], tok_send, tok_recv, ring.sibling)
    toks_total.wait_recv()
    toks_total.wait_send()
    wt_copy.wait()
    for g in (last - 1, last):
        z_out(g, g % 2).wait()
        h_out(g, g % 2).wait()
    lse_total = hop(lse_ref.at[everyone], lse_ref.at[everyone], lse_send, lse_recv, ring.sibling)
    lse_total.wait_recv()
    lse_total.wait_send()


def gather_logits(n, x, gain, bias, toks, w):
    rows, dim = x.shape
    cols = w.shape[1]
    vmem = pl.BlockSpec(memory_space=pltpu.VMEM)
    hbm = pl.BlockSpec(memory_space=pltpu.HBM)
    dma = pltpu.SemaphoreType.DMA
    return pl.pallas_call(
        functools.partial(gather_kernel, n),
        out_shape=(
            jax.ShapeDtypeStruct((n, rows, dim), BF16),
            jax.ShapeDtypeStruct((n, rows, cols), F32),
            jax.ShapeDtypeStruct((cols, dim), BF16),
            jax.ShapeDtypeStruct((n, 1, rows), F32),
            jax.ShapeDtypeStruct((n, 1, 2 * rows), F32),
        ),
        in_specs=[vmem, vmem, vmem, vmem, hbm],
        out_specs=(hbm, hbm, hbm, vmem, vmem),
        scratch_shapes=[
            pltpu.VMEM((dim, cols), BF16),
            pltpu.VMEM((cols, dim), BF16),
            pltpu.VMEM((n, rows, dim), BF16),
            pltpu.VMEM((2, rows, cols), F32),
            pltpu.VMEM((rows // 2, 128), F32),
            pltpu.VMEM((n, 2, 1, rows // 2), F32),
            pltpu.VMEM((n, 4, 1, rows // 2), F32),
            pltpu.VMEM((1, rows), F32),
            dma, dma, dma((2,)), dma((2,)), dma((4, 2, 2)), dma((4, 2, 2)), dma((2, 2)), dma((n, 2, 2)), dma((n, 2, 2)),
            dma, dma, dma, dma, dma, dma,
        ],
        compiler_params=pltpu.CompilerParams(collective_id=0, has_side_effects=True, vmem_limit_bytes=GATHER_VMEM),
        name="gather_logits",
    )(x, gain.reshape(1, dim), bias.reshape(1, dim), toks, w)


SLOTS = 8
LAG = 2
PIECES = 4
SCATTER_VMEM = 36_000_000


def scatter_kernel(n, z_hbm, h_hbm, w_hbm, lse_ref, toks_ref, dw, dh_ref, t_ref,
                   w_v, zb, hb, dzb, part, from_x, from_s, from_d, flat, cols, w_sem, z_sem, h_sem,
                   send_x, send_s, send_d, recv_x, recv_s, recv_d, credit_x, credit_s):
    ring = Rings(n)
    rows, dim = dh_ref.shape
    vocab = w_v.shape[0]
    half, quart, wide = rows // 2, rows // 4, dim // PIECES
    xo = pl.multiple_of(half * ring.core, half)
    so = pl.multiple_of(half * (1 - ring.core), half)
    col_start = ring.me * vocab

    ring.greet()

    def fetch(hbm, buf, sem, j, slot):
        return [
            pltpu.make_async_copy(
                hbm.at[lax.rem(j + ahead, n), pl.ds(off, half)], buf.at[slot, pl.ds(off, half)], sem.at[slot, ahead])
            for ahead, off in ((0, xo), (1, so))
        ]

    w_copy = pltpu.make_async_copy(w_hbm, w_v, w_sem)
    for copy in fetch(z_hbm, zb, z_sem, 1, 0) + [w_copy] + fetch(h_hbm, hb, h_sem, 1, 0) + fetch(z_hbm, zb, z_sem, 2, 1):
        copy.start()

    mask_total = jnp.sum(jnp.sum(toks_ref[:, :, rows:], axis=0), axis=-1, keepdims=True)
    flat[...] = jnp.zeros_like(flat)
    t_ref[...] = jnp.zeros_like(t_ref)

    def columns(j):
        valid = jnp.where(j <= n, 1.0, 0.0)
        for q in range(4):
            group = lax.rem(jnp.where(ring.core == q // 2, j, j + 1), n)
            who = ring.owner(group, q)
            lanes = slice(q * quart, (q + 1) * quart)
            flat[0:1, lanes] = toks_ref[who][:, lanes] - col_start.astype(F32)
            flat[1:2, lanes] = toks_ref[who][:, rows + q * quart:rows + (q + 1) * quart] * valid / mask_total
            flat[2:3, lanes] = lse_ref[who][:, lanes]
        cols[...] = jnp.transpose(flat[...])

    dz_rows = min(16, quart)

    def make_dz(slot, u):
        for b in range(rows // PIECES // dz_rows):
            r = slice(u * (rows // PIECES) + b * dz_rows, u * (rows // PIECES) + (b + 1) * dz_rows)
            z = zb[slot, r, :]
            label = cols[r, 0:1].astype(jnp.int32)
            weight = cols[r, 1:2]
            prob = jnp.exp(z - cols[r, 2:3])
            hit = lax.broadcasted_iota(jnp.int32, z.shape, 1) == label
            dzb[slot, r, :] = (jnp.where(hit, prob - 1.0, prob) * weight).astype(BF16)
            taken = jnp.where(hit, z * weight, 0.0)
            acc = taken[:, 0:128]
            for v in range(1, vocab // 128):
                acc = acc + taken[:, v * 128:(v + 1) * 128]
            t_ref[...] += acc

    def matmuls(now, u, slot):
        dz = dzb[now]
        d = slice(u * wide, (u + 1) * wide)
        part[slot] = jnp.dot(dz, w_v[:, d], preferred_element_type=F32)
        dw[d, :] += lax.dot_general(hb[now, :, d], dz, (((0,), (0,)), ((), ())), preferred_element_type=F32)

    def hop(src, dst, send_sem, recv_sem, who):
        return pltpu.make_async_remote_copy(
            src_ref=src, dst_ref=dst, send_sem=send_sem, recv_sem=recv_sem,
            device_id={"vp": who}, device_id_type=MESH)

    def x_rows(c):
        return pl.ds(xo + c * quart, quart)

    def s_rows(c):
        return pl.ds(so + c * quart, quart)

    def x_copy(slot, c):
        return hop(part.at[slot, x_rows(c)], from_s.at[slot, c], send_x.at[slot, c], recv_s.at[slot, c], ring.sibling)

    def s_copy(slot, c):
        return hop(part.at[slot, s_rows(c)], from_x.at[slot, c], send_s.at[slot, c], recv_x.at[slot, c], ring.s_next[c])

    def d_copy(slot, u, c):
        return hop(part.at[slot, s_rows(c)], from_d.at[u, c], send_d.at[u, c], recv_d.at[u, c], ring.sibling)

    first, end = PIECES, PIECES * n

    def do_x(j, k, slot):
        @pl.when((k >= first + SLOTS) & (k < end))
        def _():
            for c in range(2):
                s_copy(slot, c).wait_recv()
                part[slot, x_rows(c), :] += from_x[slot, c]

        @pl.when((k >= first + SLOTS) & (k < end - PIECES))
        def _():
            for c in range(2):
                pl.semaphore_signal(credit_s.at[c], inc=1, device_id={"vp": ring.s_next[c]}, device_id_type=MESH)

        @pl.when(k < end)
        def _():
            for c in range(2):
                @pl.when(k >= first + SLOTS)
                def _():
                    pl.semaphore_wait(credit_x.at[c], 1)
                x_copy(slot, c).start()

    def do_s(k, slot, u):
        @pl.when((k >= first) & (k < end))
        def _():
            for c in range(2):
                x_copy(slot, c).wait_recv()
                part[slot, s_rows(c), :] += from_s[slot, c]

        @pl.when((k >= first) & (k < end - SLOTS))
        def _():
            for c in range(2):
                pl.semaphore_signal(credit_x.at[c], inc=1, device_id={"vp": ring.sibling}, device_id_type=MESH)

        @pl.when((k >= first) & (k < end - PIECES))
        def _():
            for c in range(2):
                @pl.when(k >= first + SLOTS)
                def _():
                    pl.semaphore_wait(credit_s.at[c], 1)
                s_copy(slot, c).start()

        @pl.when((k >= end - PIECES) & (k < end))
        def _():
            dh_ref[pl.ds(so, half), u * wide:(u + 1) * wide] = part[slot, pl.ds(so, half), :]

    dw[...] = jnp.zeros_like(dw)
    columns(1)
    for copy in fetch(z_hbm, zb, z_sem, 1, 0):
        copy.wait()
    for u in range(PIECES):
        make_dz(0, u)
    for copy in fetch(h_hbm, hb, h_sem, 1, 0):
        copy.wait()
    w_copy.wait()
    ring.greeted()

    @pl.loop(0, n // 2)
    def _(a):
        for b in range(2):
            j = 2 * a + b + 1
            now, then = b, 1 - b

            @pl.when(j < n)
            def _():
                for copy in fetch(z_hbm, zb, z_sem, j + 1, then):
                    copy.wait()
                for copy in fetch(h_hbm, hb, h_sem, j + 1, then):
                    copy.start()

            @pl.when(j < n - 1)
            def _():
                for copy in fetch(z_hbm, zb, z_sem, j + 2, now):
                    copy.start()

            columns(j + 1)
            for u in range(PIECES):
                k = PIECES * j + u
                slot = (PIECES * (b + 1) + u) % SLOTS

                @pl.when(k >= first + SLOTS)
                def _():
                    for c in range(2):
                        x_copy(slot, c).wait_send()
                        s_copy(slot, c).wait_send()

                matmuls(now, u, slot)
                make_dz(then, u)

                @pl.when(j == n)
                def _():
                    for c in range(2):
                        d_copy(slot, u, c).start()

                do_x(j, k, slot)
                do_s(k - LAG, (slot - LAG) % SLOTS, (u - LAG) % PIECES)

            @pl.when(j < n)
            def _():
                for copy in fetch(h_hbm, hb, h_sem, j + 1, then):
                    copy.wait()

    for u in range(PIECES):
        slot = (end + u) % SLOTS
        for c in range(2):
            d_copy(slot, u, c).wait_recv()
            s_copy(slot, c).wait_recv()
            dh_ref[x_rows(c), u * wide:(u + 1) * wide] = part[slot, x_rows(c), :] + from_d[u, c] + from_x[slot, c]
    for u in range(PIECES):
        for c in range(2):
            x_copy((end - PIECES + u) % SLOTS, c).wait_send()
            d_copy((end + u) % SLOTS, u, c).wait_send()


def scatter_grads(n, z, h, w, lse, toks):
    _, rows, vocab = z.shape
    dim = w.shape[1]
    vmem = pl.BlockSpec(memory_space=pltpu.VMEM)
    hbm = pl.BlockSpec(memory_space=pltpu.HBM)
    dma = pltpu.SemaphoreType.DMA
    wide = dim // PIECES
    return pl.pallas_call(
        functools.partial(scatter_kernel, n),
        out_shape=(
            pltpu.VMEM((dim, vocab), F32),
            pltpu.VMEM((rows, dim), F32),
            pltpu.VMEM((16, 128), F32),
        ),
        in_specs=[hbm, hbm, hbm, vmem, vmem],
        out_specs=(vmem, vmem, vmem),
        scratch_shapes=[
            pltpu.VMEM((vocab, dim), BF16),
            pltpu.VMEM((2, rows, vocab), F32),
            pltpu.VMEM((2, rows, dim), BF16),
            pltpu.VMEM((2, rows, vocab), BF16),
            pltpu.VMEM((SLOTS, rows, wide), F32),
            pltpu.VMEM((SLOTS, 2, rows // 4, wide), F32),
            pltpu.VMEM((SLOTS, 2, rows // 4, wide), F32),
            pltpu.VMEM((PIECES, 2, rows // 4, wide), F32),
            pltpu.VMEM((128, rows), F32),
            pltpu.VMEM((rows, 128), F32),
            dma, dma((2, 2)), dma((2, 2)),
            dma((SLOTS, 2)), dma((SLOTS, 2)), dma((PIECES, 2)), dma((SLOTS, 2)), dma((SLOTS, 2)), dma((PIECES, 2)),
            pltpu.SemaphoreType.REGULAR((2,)),
            pltpu.SemaphoreType.REGULAR((2,)),
        ],
        compiler_params=pltpu.CompilerParams(collective_id=1, has_side_effects=True, vmem_limit_bytes=SCATTER_VMEM),
        name="scatter_grads",
    )(z, h, w, lse, toks)


def local_kernel(dh_ref, x_ref, gain_ref, t_ref, dw_ref, dx_ref, sums_ref, dw_hbm, dw_sem):
    rows, dim = dh_ref.shape
    blk = min(64, rows)
    dw_copy = pltpu.make_async_copy(dw_ref, dw_hbm, dw_sem)
    dw_copy.start()

    def body(b, carry):
        dg, dc = carry
        r = pl.ds(pl.multiple_of(b * blk, blk), blk)
        normed, inv_std = norm_rows(x_ref[r, :])
        dh = dh_ref[r, :]
        dhn = dh * normed
        scaled = dh * (1.0 + gain_ref[...])
        mean_s = jnp.mean(scaled, axis=-1, keepdims=True)
        mean_sn = jnp.mean(scaled * normed, axis=-1, keepdims=True)
        dx_ref[r, :] = (inv_std * (scaled - mean_s - normed * mean_sn)).astype(BF16)
        return dg + jnp.sum(dhn, axis=0, keepdims=True), dc + jnp.sum(dh, axis=0, keepdims=True)

    zero = jnp.zeros((1, dim), F32)
    dg, dc = lax.fori_loop(0, rows // blk, body, (zero, zero))
    sums_ref[0, :, 0:dim] = dg
    sums_ref[1, :, 0:dim] = dc
    sums_ref[0, :, dim:] = jnp.sum(t_ref[...], axis=0, keepdims=True)
    sums_ref[1, :, dim:] = jnp.zeros((1, 128), F32)
    dw_copy.wait()


def local_backward(dh, x, gain, t, dw):
    rows, dim = dh.shape
    vmem = pl.BlockSpec(memory_space=pltpu.VMEM)
    return pl.pallas_call(
        local_kernel,
        out_shape=(
            jax.ShapeDtypeStruct((rows, dim), BF16),
            jax.ShapeDtypeStruct((2, 1, dim + 128), F32),
            jax.ShapeDtypeStruct(dw.shape, F32),
        ),
        in_specs=[vmem] * 5,
        out_specs=(vmem, vmem, pl.BlockSpec(memory_space=pltpu.HBM)),
        scratch_shapes=[pltpu.SemaphoreType.DMA],
        compiler_params=pltpu.CompilerParams(vmem_limit_bytes=24_000_000),
        name="local_backward",
    )(dh, x, gain.reshape(1, dim), t, dw)


def sums_kernel(n, mine_ref, lse_ref, toks_ref, dg_ref, dc_ref, loss_ref,
                near, both, chips, total, send_a, recv_a, send_b, recv_b, send_c, recv_c):
    me = lax.axis_index("vp")
    core, chip = lax.rem(me, 2), lax.div(me, 2)
    count = n // 2
    sibling = me + 1 - 2 * core
    dim = dg_ref.shape[1]
    rows = lse_ref.shape[-1]

    def peer(d):
        return 2 * lax.rem(chip + d, count) + core

    barrier = pltpu.get_barrier_semaphore()
    pl.semaphore_signal(barrier, inc=1, device_id={"vp": sibling}, device_id_type=MESH)
    for d in range(1, count):
        pl.semaphore_signal(barrier, inc=1, device_id={"vp": peer(d)}, device_id_type=MESH)

    mask = toks_ref[:, :, rows:]
    mask_total = jnp.sum(jnp.sum(mask, axis=0), axis=-1, keepdims=True)
    lse_sum = jnp.sum(jnp.sum(lse_ref[...] * (mask / mask_total[None]), axis=0), axis=-1, keepdims=True)
    pl.semaphore_wait(barrier, count)

    def hop(src, dst, send_sem, recv_sem, who):
        return pltpu.make_async_remote_copy(
            src_ref=src, dst_ref=dst, send_sem=send_sem, recv_sem=recv_sem,
            device_id={"vp": who}, device_id_type=MESH)

    first = hop(mine_ref, near, send_a, recv_a, sibling)
    first.start()
    first.wait_recv()
    both[...] = mine_ref[core] + near[core]

    def second(d):
        return hop(both, chips.at[chip], send_b.at[d], recv_b.at[d], peer(d))

    @pl.loop(1, count)
    def _(d):
        second(d).start()

    chips[chip] = both[...]

    @pl.loop(1, count)
    def _(d):
        second(d).wait()

    total[core] = jnp.sum(chips[...], axis=0)
    third = hop(total.at[core], total.at[core], send_c, recv_c, sibling)
    third.start()
    first.wait_send()
    third.wait()
    dg_ref[...] = total[0, :, 0:dim]
    dc_ref[...] = total[1, :, 0:dim]
    loss_ref[...] = lse_sum - jnp.sum(total[0, :, dim:], axis=-1, keepdims=True)


def group_sums(n, mine, lse, toks):
    wide = mine.shape[-1]
    dim = wide - 128
    vmem = pl.BlockSpec(memory_space=pltpu.VMEM)
    dma = pltpu.SemaphoreType.DMA
    return pl.pallas_call(
        functools.partial(sums_kernel, n),
        out_shape=(
            jax.ShapeDtypeStruct((1, dim), F32),
            jax.ShapeDtypeStruct((1, dim), F32),
            jax.ShapeDtypeStruct((1, 1), F32),
        ),
        in_specs=[vmem] * 3,
        out_specs=(vmem,) * 3,
        scratch_shapes=[
            pltpu.VMEM((2, 1, wide), F32),
            pltpu.VMEM((1, wide), F32),
            pltpu.VMEM((n // 2, 1, wide), F32),
            pltpu.VMEM((2, 1, wide), F32),
            dma, dma, dma((n // 2,)), dma((n // 2,)), dma, dma,
        ],
        compiler_params=pltpu.CompilerParams(collective_id=2, has_side_effects=True, vmem_limit_bytes=16_000_000),
        name="group_sums",
    )(mine, lse, toks)


def solution(mesh):
    n = mesh.shape["vp"]

    def per_device(hidden, norm_gain, norm_bias, w_blk, labels, loss_mask):
        dim = hidden.shape[-1]
        x = hidden.reshape(-1, dim)
        rows = x.shape[0]
        toks_mine = jnp.concatenate([labels.reshape(1, rows).astype(F32), loss_mask.reshape(1, rows)], axis=1)
        h, z, wt, lse, toks = gather_logits(n, x, norm_gain, norm_bias, toks_mine, w_blk)
        dw, dh, t = scatter_grads(n, z, h, wt, lse, toks)
        grad_x, sums, grad_w = local_backward(dh, x, norm_gain, t, dw)
        grad_gain, grad_bias, loss = group_sums(n, sums, lse, toks)
        return loss.reshape(1), grad_x.reshape(hidden.shape), grad_w, grad_gain.reshape(dim), grad_bias.reshape(dim)

    tok_spec = P("vp", "dp")
    return jax.shard_map(
        per_device,
        mesh=mesh,
        in_specs=(P("vp", "dp", None), P(None), P(None), P(None, "vp"), tok_spec, tok_spec),
        out_specs=(P("dp"), P("vp", "dp", None), P("dp", "vp"), P("dp"), P("dp")),
        check_vma=False,
    )
```

```python
import functools
import math

import jax
import jax.numpy as jnp
from jax import lax
from jax.experimental import pallas as pl
from jax.experimental.pallas import tpu as pltpu
from jax.sharding import PartitionSpec as P

NORM_EPS = 1e-5
MESH = pl.DeviceIdType.MESH
GATHER_VMEM = 62_000_000
F32 = jnp.float32
BF16 = jnp.bfloat16


class Rings:
    def __init__(self, n):
        self.n = n
        self.chips = n // 2
        self.side = math.isqrt(self.chips)
        assert self.side * self.side * 2 == n
        self.me = lax.axis_index("vp")
        self.core = lax.rem(self.me, 2)
        chip = lax.div(self.me, 2)
        x, y = lax.rem(chip, self.side), lax.div(chip, self.side)
        k = lax.rem(x + y, self.side)
        self.spot = (y * self.side + k, x * self.side + k)
        self.sibling = self.me + 1 - 2 * self.core
        step = 2 * self.core - 1
        self.s_next = [self.at(c, lax.rem(self.spot[c] + step + self.chips, self.chips), 1 - self.core) for c in range(2)]
        self.x_prev = [self.at(c, lax.rem(self.spot[c] + step + self.chips, self.chips), 1 - self.core) for c in range(2)]

    def at(self, cycle, spot, core):
        q, k = lax.div(spot, self.side), lax.rem(spot, self.side)
        a = lax.rem(k - q + self.side, self.side)
        chip = q * self.side + a if cycle == 0 else a * self.side + q
        return chip * 2 + core

    def owner(self, group, quarter):
        cycle = quarter % 2
        pos = 2 * self.spot[cycle] + self.core
        shift = self.n - group if quarter < 2 else group
        origin = lax.rem(pos + shift + self.n, self.n)
        return self.at(cycle, lax.div(origin, 2), lax.rem(origin, 2))

    def greet(self):
        barrier = pltpu.get_barrier_semaphore()
        for other in (self.sibling, *self.s_next):
            pl.semaphore_signal(barrier, inc=1, device_id={"vp": other}, device_id_type=MESH)

    def greeted(self):
        pl.semaphore_wait(pltpu.get_barrier_semaphore(), 3)


def norm_rows(x_rows):
    x = x_rows.astype(F32)
    centered = x - jnp.mean(x, axis=-1, keepdims=True)
    inv_std = lax.rsqrt(jnp.mean(centered * centered, axis=-1, keepdims=True) + NORM_EPS)
    return centered * inv_std, inv_std


def signal_all(n, me):
    barrier = pltpu.get_barrier_semaphore()
    for d in range(1, n):
        pl.semaphore_signal(barrier, inc=1, device_id={"vp": lax.rem(me + d, n)}, device_id_type=MESH)


def gather_kernel(n, x_ref, gain_ref, bias_ref, label_ref, mask_ref, w_hbm, h_hbm, z_hbm, wt_hbm, lse_ref, toks_ref,
                  w_v, wt_v, h_all, zbuf, col, local, got, own, tok_ref, w_sem, wt_sem, h_sem, z_sem, send_x, send_s, send_d, recv_x, recv_s,
                  stat_send, stat_recv, lse_send, lse_recv, tok_send, tok_recv):
    ring = Rings(n)
    me = ring.me
    rows, dim = x_ref.shape
    cols = w_v.shape[1]
    half, quart, piece, wide = rows // 2, rows // 4, rows // 8, cols // 2
    xo = pl.multiple_of(half * ring.core, half)
    so = pl.multiple_of(half * (1 - ring.core), half)

    w_copy = pltpu.make_async_copy(w_hbm, w_v, w_sem)
    w_copy.start()
    signal_all(n, me)

    ln_rows = min(64, half)

    def norm_half(base):
        @pl.loop(0, half // ln_rows)
        def _(b):
            r = pl.ds(pl.multiple_of(base + b * ln_rows, ln_rows), ln_rows)
            normed, _ = norm_rows(x_ref[r, :])
            h_all[0, r, :] = (normed * (1.0 + gain_ref[...]) + bias_ref[...]).astype(BF16)

    norm_half(so)
    pl.semaphore_wait(pltpu.get_barrier_semaphore(), n - 1)

    def hop(src, dst, send_sem, recv_sem, who):
        return pltpu.make_async_remote_copy(
            src_ref=src, dst_ref=dst, send_sem=send_sem, recv_sem=recv_sem,
            device_id={"vp": who}, device_id_type=MESH)

    def x_copy(i, c, u):
        r = pl.ds(xo + (c * quart + u * piece), piece)
        return hop(h_all.at[i, r], h_all.at[i + 1, r], send_x.at[lax.rem(i, 4), c, u], recv_s.at[i + 1, c, u], ring.sibling)

    def s_copy(i, c, u):
        r = pl.ds(so + (c * quart + u * piece), piece)
        return hop(h_all.at[i, r], h_all.at[i + 1, r], send_s.at[lax.rem(i, 4), c, u], recv_x.at[i + 1, c, u], ring.s_next[c])

    def d_copy(c, u):
        r = pl.ds(so + (c * quart + u * piece), piece)
        return hop(h_all.at[0, r], h_all.at[n - 1, r], send_d.at[c, u], recv_x.at[n - 1, c, u], ring.sibling)

    for c in range(2):
        s_copy(0, c, 0).start()
    norm_half(xo)

    def x_arrived(i, c, u):
        r = pl.ds(xo + (c * quart + u * piece), piece)
        hop(h_all.at[i, r], h_all.at[i, r], send_s.at[0, c, u], recv_x.at[i, c, u], ring.s_next[c]).wait_recv()

    def s_arrived(i, c, u):
        r = pl.ds(so + (c * quart + u * piece), piece)
        hop(h_all.at[i, r], h_all.at[i, r], send_x.at[0, c, u], recv_s.at[i, c, u], ring.sibling).wait_recv()

    def send(copy, i, c, u):
        @pl.when(i >= 4)
        def _():
            copy(i - 4, c, u).wait_send()
        copy(i, c, u).start()

    def z_out(g, slot):
        return pltpu.make_async_copy(zbuf.at[slot], z_hbm.at[g], z_sem.at[slot])

    def h_out(g, slot):
        return pltpu.make_async_copy(h_all.at[g], h_hbm.at[g], h_sem.at[slot])

    stat_rows = min(32, half)

    def stats(slot, u):
        for b in range(half // stat_rows):
            z = zbuf[slot, u * half + b * stat_rows:u * half + (b + 1) * stat_rows, :]
            top = jnp.max(z, axis=-1, keepdims=True)
            lse = top + jnp.log(jnp.sum(jnp.exp(z - top), axis=-1, keepdims=True))
            col[b * stat_rows:(b + 1) * stat_rows, :] = jnp.broadcast_to(lse, (stat_rows, col.shape[1]))
        return jnp.transpose(col[...])[0:1, :]

    def stat_copy(g, u, c):
        q = 2 * u + c
        return hop(local.at[g, u], got.at[g, q], stat_send, stat_recv, ring.owner(g, q))

    def send_stats(g):
        for u in range(2):
            for c in range(2):
                stat_copy(g, u, c).start()

    def logits(g, slot, u):
        part = slice(u * wide, (u + 1) * wide)
        zbuf[slot, :, part] = jnp.dot(h_all[g], w_v[:, part], preferred_element_type=F32)

    strip = dim // n

    def flip(a, b):
        r = pl.ds(pl.multiple_of(a * (2 * strip), 2 * strip), 2 * strip)
        part = slice(b * wide, (b + 1) * wide)
        wt_v[part, r] = jnp.transpose(w_v[r, part])

    def tok_copy(d):
        return hop(tok_ref, toks_ref.at[me], tok_send, tok_recv, lax.rem(me + d, n))

    def lse_copy(d):
        return hop(own, lse_ref.at[me], lse_send, lse_recv, lax.rem(me + d, n))

    outer, inner = label_ref.shape

    def in_line(block):
        lane = lax.broadcasted_iota(jnp.int32, (inner, rows), 1)
        spread = (lax.rem(lane, inner) == lax.broadcasted_iota(jnp.int32, (inner, rows), 0)).astype(F32)
        line = lax.div(lax.broadcasted_iota(jnp.int32, (outer, rows), 1), inner)
        chosen = line == lax.broadcasted_iota(jnp.int32, (outer, rows), 0)
        return jnp.sum(jnp.where(chosen, jnp.dot(block, spread, preferred_element_type=F32), 0.0), axis=0, keepdims=True)

    def tokens():
        label = label_ref[...]
        high = in_line(lax.shift_right_logical(label, 8).astype(F32))
        tok_ref[:, :rows] = 256.0 * high + in_line((label & 255).astype(F32))
        tok_ref[:, rows:] = in_line(mask_ref[...])

    zbuf[...] = jnp.zeros_like(zbuf)
    w_copy.wait()

    @pl.loop(0, n // 2)
    def _(a):
        for b in range(2):
            i = 2 * a + b
            for u in range(2):
                @pl.when(i >= 1)
                def _():
                    for c in range(2):
                        x_arrived(i, c, u)

                @pl.when(i < n - 1)
                def _():
                    for c in range(2):
                        send(x_copy, i, c, u)

                j = i + u

                @pl.when((j >= 1) & (j < n))
                def _():
                    for c in range(2):
                        s_arrived(j, c, 1 - u)

                @pl.when(j < n - 2)
                def _():
                    for c in range(2):
                        send(s_copy, j, c, 1 - u)

                if u == 0:
                    flip(a, b)
                else:
                    @pl.when(i == 0)
                    def _():
                        for c in range(2):
                            for v in range(2):
                                d_copy(c, v).start()

                        tokens()

                    @pl.when(i == 2)
                    def _():
                        @pl.loop(1, n)
                        def _(d):
                            tok_copy(d).start()

                    @pl.when(i >= 3)
                    def _():
                        send_stats(i - 2)

                if u == 0:
                    @pl.when(i >= 1)
                    def _():
                        logits(i - 1, 1 - b, 1)
                        local[lax.max(i - 2, 0), 1] = stats(b, 1)
                        z_out(i - 1, 1 - b).start()
                else:
                    @pl.when(i >= 2)
                    def _():
                        z_out(i - 2, b).wait()
                        h_out(i - 2, b).wait()
                    h_out(i, b).start()
                    logits(i, b, 0)
                    local[lax.max(i - 1, 0), 0] = stats(1 - b, 0)

    last = n - 1
    wt_copy = pltpu.make_async_copy(wt_v, wt_hbm, wt_sem)
    wt_copy.start()
    logits(last, 1, 1)
    local[last - 1, 1] = stats(0, 1)
    z_out(last, 1).start()
    for u in range(2):
        local[last, u] = stats(1, u)
    send_stats(last - 1)
    send_stats(last)
    for q in range(4):
        got[0, q] = local[0, q // 2]
    toks_ref[me] = tok_ref[...]

    everyone = pl.ds(1, n - 1)
    stats_total = hop(got.at[everyone], got.at[everyone], stat_send, stat_recv, ring.sibling)
    stats_total.wait_recv()
    for q in range(4):
        parts = got[:, q]
        top = jnp.max(parts, axis=0)
        lse = top + jnp.log(jnp.sum(jnp.exp(parts - top[None]), axis=0))
        lanes = slice((q % 2) * quart, (q % 2 + 1) * quart)
        own[:, q * quart:(q + 1) * quart] = lse[:, lanes]
    lse_ref[me] = own[...]

    @pl.loop(1, n)
    def _(d):
        lse_copy(d).start()

    for c in range(2):
        for u in range(2):
            d_copy(c, u).wait_send()
            for i in range(n - 5, n - 1):
                x_copy(i, c, u).wait_send()
            for i in range(n - 6, n - 2):
                s_copy(i, c, u).wait_send()
    stats_total.wait_send()
    toks_total = hop(toks_ref.at[everyone], toks_ref.at[everyone], tok_send, tok_recv, ring.sibling)
    toks_total.wait_recv()
    toks_total.wait_send()
    wt_copy.wait()
    for g in (last - 1, last):
        z_out(g, g % 2).wait()
        h_out(g, g % 2).wait()
    lse_total = hop(lse_ref.at[everyone], lse_ref.at[everyone], lse_send, lse_recv, ring.sibling)
    lse_total.wait_recv()
    lse_total.wait_send()


def gather_logits(n, x, gain, bias, labels, mask, w):
    rows, dim = x.shape
    cols = w.shape[1]
    vmem = pl.BlockSpec(memory_space=pltpu.VMEM)
    hbm = pl.BlockSpec(memory_space=pltpu.HBM)
    dma = pltpu.SemaphoreType.DMA
    return pl.pallas_call(
        functools.partial(gather_kernel, n),
        out_shape=(
            jax.ShapeDtypeStruct((n, rows, dim), BF16),
            jax.ShapeDtypeStruct((n, rows, cols), F32),
            jax.ShapeDtypeStruct((cols, dim), BF16),
            jax.ShapeDtypeStruct((n, 1, rows), F32),
            jax.ShapeDtypeStruct((n, 1, 2 * rows), F32),
        ),
        in_specs=[vmem, vmem, vmem, vmem, vmem, hbm],
        out_specs=(hbm, hbm, hbm, vmem, vmem),
        scratch_shapes=[
            pltpu.VMEM((dim, cols), BF16),
            pltpu.VMEM((cols, dim), BF16),
            pltpu.VMEM((n, rows, dim), BF16),
            pltpu.VMEM((2, rows, cols), F32),
            pltpu.VMEM((rows // 2, 128), F32),
            pltpu.VMEM((n, 2, 1, rows // 2), F32),
            pltpu.VMEM((n, 4, 1, rows // 2), F32),
            pltpu.VMEM((1, rows), F32),
            pltpu.VMEM((1, 2 * rows), F32),
            dma, dma, dma((2,)), dma((2,)), dma((4, 2, 2)), dma((4, 2, 2)), dma((2, 2)), dma((n, 2, 2)), dma((n, 2, 2)),
            dma, dma, dma, dma, dma, dma,
        ],
        compiler_params=pltpu.CompilerParams(collective_id=0, has_side_effects=True, vmem_limit_bytes=GATHER_VMEM),
        name="gather_logits",
    )(x, gain.reshape(1, dim), bias.reshape(1, dim), labels, mask, w)


SLOTS = 8
LAG = 2
PIECES = 4
SCATTER_VMEM = 36_000_000


def scatter_kernel(n, z_hbm, h_hbm, w_hbm, lse_hbm, toks_hbm, dw, dh_ref, t_ref,
                   lse_ref, toks_ref, tok_sem, w_v, zb, hb, dzb, part, from_x, from_s, from_d, flat, cols, w_sem, z_sem, h_sem,
                   send_x, send_s, send_d, recv_x, recv_s, recv_d, credit_x, credit_s):
    ring = Rings(n)
    rows, dim = dh_ref.shape
    vocab = w_v.shape[0]
    half, quart, wide = rows // 2, rows // 4, dim // PIECES
    xo = pl.multiple_of(half * ring.core, half)
    so = pl.multiple_of(half * (1 - ring.core), half)
    col_start = ring.me * vocab

    ring.greet()

    def fetch(hbm, buf, sem, j, slot):
        return [
            pltpu.make_async_copy(
                hbm.at[lax.rem(j + ahead, n), pl.ds(off, half)], buf.at[slot, pl.ds(off, half)], sem.at[slot, ahead])
            for ahead, off in ((0, xo), (1, so))
        ]

    w_copy = pltpu.make_async_copy(w_hbm, w_v, w_sem)
    tok_copies = [pltpu.make_async_copy(lse_hbm, lse_ref, tok_sem.at[0]), pltpu.make_async_copy(toks_hbm, toks_ref, tok_sem.at[1])]
    for copy in tok_copies + fetch(z_hbm, zb, z_sem, 1, 0) + [w_copy] + fetch(h_hbm, hb, h_sem, 1, 0) + fetch(z_hbm, zb, z_sem, 2, 1):
        copy.start()

    flat[...] = jnp.zeros_like(flat)
    dw[...] = jnp.zeros_like(dw)
    for copy in tok_copies:
        copy.wait()
    mask_total = jnp.sum(jnp.sum(toks_ref[:, :, rows:], axis=0), axis=-1, keepdims=True)
    lse_term = jnp.sum(lse_ref[ring.me] * (toks_ref[ring.me][:, rows:] / mask_total), axis=-1, keepdims=True)
    corner = (lax.broadcasted_iota(jnp.int32, t_ref.shape, 0) == 0) & (lax.broadcasted_iota(jnp.int32, t_ref.shape, 1) == 0)
    t_ref[...] = jnp.where(corner, -lse_term, 0.0)

    def columns(j):
        valid = jnp.where(j <= n, 1.0, 0.0)
        for q in range(4):
            group = lax.rem(jnp.where(ring.core == q // 2, j, j + 1), n)
            who = ring.owner(group, q)
            lanes = slice(q * quart, (q + 1) * quart)
            flat[0:1, lanes] = toks_ref[who][:, lanes] - col_start.astype(F32)
            flat[1:2, lanes] = toks_ref[who][:, rows + q * quart:rows + (q + 1) * quart] * valid / mask_total
            flat[2:3, lanes] = lse_ref[who][:, lanes]
        cols[...] = jnp.transpose(flat[...])

    dz_rows = min(16, quart)

    def make_dz(slot, u):
        for b in range(rows // PIECES // dz_rows):
            r = slice(u * (rows // PIECES) + b * dz_rows, u * (rows // PIECES) + (b + 1) * dz_rows)
            z = zb[slot, r, :]
            label = cols[r, 0:1].astype(jnp.int32)
            weight = cols[r, 1:2]
            prob = jnp.exp(z - cols[r, 2:3])
            hit = lax.broadcasted_iota(jnp.int32, z.shape, 1) == label
            dzb[slot, r, :] = (jnp.where(hit, prob - 1.0, prob) * weight).astype(BF16)
            taken = jnp.where(hit, z * weight, 0.0)
            acc = taken[:, 0:128]
            for v in range(1, vocab // 128):
                acc = acc + taken[:, v * 128:(v + 1) * 128]
            t_ref[...] += acc

    def matmuls(now, u, slot):
        dz = dzb[now]
        d = slice(u * wide, (u + 1) * wide)
        part[slot] = jnp.dot(dz, w_v[:, d], preferred_element_type=F32)
        dw[d, :] += lax.dot_general(hb[now, :, d], dz, (((0,), (0,)), ((), ())), preferred_element_type=F32)

    def hop(src, dst, send_sem, recv_sem, who):
        return pltpu.make_async_remote_copy(
            src_ref=src, dst_ref=dst, send_sem=send_sem, recv_sem=recv_sem,
            device_id={"vp": who}, device_id_type=MESH)

    def x_rows(c):
        return pl.ds(xo + c * quart, quart)

    def s_rows(c):
        return pl.ds(so + c * quart, quart)

    def x_copy(slot, c):
        return hop(part.at[slot, x_rows(c)], from_s.at[slot, c], send_x.at[slot, c], recv_s.at[slot, c], ring.sibling)

    def s_copy(slot, c):
        return hop(part.at[slot, s_rows(c)], from_x.at[slot, c], send_s.at[slot, c], recv_x.at[slot, c], ring.s_next[c])

    def d_copy(slot, u, c):
        return hop(part.at[slot, s_rows(c)], from_d.at[u, c], send_d.at[u, c], recv_d.at[u, c], ring.sibling)

    first, end = PIECES, PIECES * n

    def do_x(j, k, slot):
        @pl.when((k >= first + SLOTS) & (k < end))
        def _():
            for c in range(2):
                s_copy(slot, c).wait_recv()
                part[slot, x_rows(c), :] += from_x[slot, c]

        @pl.when((k >= first + SLOTS) & (k < end - PIECES))
        def _():
            for c in range(2):
                pl.semaphore_signal(credit_s.at[c], inc=1, device_id={"vp": ring.s_next[c]}, device_id_type=MESH)

        @pl.when(k < end)
        def _():
            for c in range(2):
                @pl.when(k >= first + SLOTS)
                def _():
                    pl.semaphore_wait(credit_x.at[c], 1)
                x_copy(slot, c).start()

    def do_s(k, slot, u):
        @pl.when((k >= first) & (k < end))
        def _():
            for c in range(2):
                x_copy(slot, c).wait_recv()
                part[slot, s_rows(c), :] += from_s[slot, c]

        @pl.when((k >= first) & (k < end - SLOTS))
        def _():
            for c in range(2):
                pl.semaphore_signal(credit_x.at[c], inc=1, device_id={"vp": ring.sibling}, device_id_type=MESH)

        @pl.when((k >= first) & (k < end - PIECES))
        def _():
            for c in range(2):
                @pl.when(k >= first + SLOTS)
                def _():
                    pl.semaphore_wait(credit_s.at[c], 1)
                s_copy(slot, c).start()

        @pl.when((k >= end - PIECES) & (k < end))
        def _():
            dh_ref[pl.ds(so, half), u * wide:(u + 1) * wide] = part[slot, pl.ds(so, half), :]

    columns(1)
    for copy in fetch(z_hbm, zb, z_sem, 1, 0):
        copy.wait()
    for u in range(PIECES):
        make_dz(0, u)
    for copy in fetch(h_hbm, hb, h_sem, 1, 0):
        copy.wait()
    w_copy.wait()
    ring.greeted()

    @pl.loop(0, n // 2)
    def _(a):
        for b in range(2):
            j = 2 * a + b + 1
            now, then = b, 1 - b

            @pl.when(j < n)
            def _():
                for copy in fetch(z_hbm, zb, z_sem, j + 1, then):
                    copy.wait()
                for copy in fetch(h_hbm, hb, h_sem, j + 1, then):
                    copy.start()

            @pl.when(j < n - 1)
            def _():
                for copy in fetch(z_hbm, zb, z_sem, j + 2, now):
                    copy.start()

            columns(j + 1)
            for u in range(PIECES):
                k = PIECES * j + u
                slot = (PIECES * (b + 1) + u) % SLOTS

                @pl.when(k >= first + SLOTS)
                def _():
                    for c in range(2):
                        x_copy(slot, c).wait_send()
                        s_copy(slot, c).wait_send()

                matmuls(now, u, slot)
                make_dz(then, u)

                @pl.when(j == n)
                def _():
                    for c in range(2):
                        d_copy(slot, u, c).start()

                do_x(j, k, slot)
                do_s(k - LAG, (slot - LAG) % SLOTS, (u - LAG) % PIECES)

            @pl.when(j < n)
            def _():
                for copy in fetch(h_hbm, hb, h_sem, j + 1, then):
                    copy.wait()

    for u in range(PIECES):
        slot = (end + u) % SLOTS
        for c in range(2):
            d_copy(slot, u, c).wait_recv()
            s_copy(slot, c).wait_recv()
            dh_ref[x_rows(c), u * wide:(u + 1) * wide] = part[slot, x_rows(c), :] + from_d[u, c] + from_x[slot, c]
    for u in range(PIECES):
        for c in range(2):
            x_copy((end - PIECES + u) % SLOTS, c).wait_send()
            d_copy((end + u) % SLOTS, u, c).wait_send()


def scatter_grads(n, z, h, w, lse, toks):
    _, rows, vocab = z.shape
    dim = w.shape[1]
    vmem = pl.BlockSpec(memory_space=pltpu.VMEM)
    hbm = pl.BlockSpec(memory_space=pltpu.HBM)
    dma = pltpu.SemaphoreType.DMA
    wide = dim // PIECES
    return pl.pallas_call(
        functools.partial(scatter_kernel, n),
        out_shape=(
            pltpu.VMEM((dim, vocab), F32),
            pltpu.VMEM((rows, dim), F32),
            pltpu.VMEM((16, 128), F32),
        ),
        in_specs=[hbm] * 5,
        out_specs=(vmem, vmem, vmem),
        scratch_shapes=[
            pltpu.VMEM(lse.shape, F32),
            pltpu.VMEM(toks.shape, F32),
            dma((2,)),
            pltpu.VMEM((vocab, dim), BF16),
            pltpu.VMEM((2, rows, vocab), F32),
            pltpu.VMEM((2, rows, dim), BF16),
            pltpu.VMEM((2, rows, vocab), BF16),
            pltpu.VMEM((SLOTS, rows, wide), F32),
            pltpu.VMEM((SLOTS, 2, rows // 4, wide), F32),
            pltpu.VMEM((SLOTS, 2, rows // 4, wide), F32),
            pltpu.VMEM((PIECES, 2, rows // 4, wide), F32),
            pltpu.VMEM((128, rows), F32),
            pltpu.VMEM((rows, 128), F32),
            dma, dma((2, 2)), dma((2, 2)),
            dma((SLOTS, 2)), dma((SLOTS, 2)), dma((PIECES, 2)), dma((SLOTS, 2)), dma((SLOTS, 2)), dma((PIECES, 2)),
            pltpu.SemaphoreType.REGULAR((2,)),
            pltpu.SemaphoreType.REGULAR((2,)),
        ],
        compiler_params=pltpu.CompilerParams(collective_id=1, has_side_effects=True, vmem_limit_bytes=SCATTER_VMEM),
        name="scatter_grads",
    )(z, h, w, pltpu.with_memory_space_constraint(lse, pltpu.HBM), pltpu.with_memory_space_constraint(toks, pltpu.HBM))


def local_kernel(dh_ref, x_ref, gain_ref, t_ref, dw_ref, dx_ref, sums_ref, dw_hbm, dw_sem):
    rows, dim = dh_ref.shape
    blk = min(64, rows)
    dw_copy = pltpu.make_async_copy(dw_ref, dw_hbm, dw_sem)
    dw_copy.start()

    def body(b, carry):
        dg, dc = carry
        r = pl.ds(pl.multiple_of(b * blk, blk), blk)
        normed, inv_std = norm_rows(x_ref[r, :])
        dh = dh_ref[r, :]
        dhn = dh * normed
        scaled = dh * (1.0 + gain_ref[...])
        mean_s = jnp.mean(scaled, axis=-1, keepdims=True)
        mean_sn = jnp.mean(scaled * normed, axis=-1, keepdims=True)
        dx_ref[r, :] = (inv_std * (scaled - mean_s - normed * mean_sn)).astype(BF16)
        return dg + jnp.sum(dhn, axis=0, keepdims=True), dc + jnp.sum(dh, axis=0, keepdims=True)

    zero = jnp.zeros((1, dim), F32)
    dg, dc = lax.fori_loop(0, rows // blk, body, (zero, zero))
    sums_ref[0, :, 0:dim] = dg
    sums_ref[1, :, 0:dim] = dc
    sums_ref[0, :, dim:] = jnp.sum(t_ref[...], axis=0, keepdims=True)
    sums_ref[1, :, dim:] = jnp.zeros((1, 128), F32)
    dw_copy.wait()


def local_backward(dh, x, gain, t, dw):
    rows, dim = dh.shape
    vmem = pl.BlockSpec(memory_space=pltpu.VMEM)
    return pl.pallas_call(
        local_kernel,
        out_shape=(
            jax.ShapeDtypeStruct((rows, dim), BF16),
            jax.ShapeDtypeStruct((2, 1, dim + 128), F32),
            jax.ShapeDtypeStruct(dw.shape, F32),
        ),
        in_specs=[vmem] * 5,
        out_specs=(vmem, vmem, pl.BlockSpec(memory_space=pltpu.HBM)),
        scratch_shapes=[pltpu.SemaphoreType.DMA],
        compiler_params=pltpu.CompilerParams(vmem_limit_bytes=24_000_000),
        name="local_backward",
    )(dh, x, gain.reshape(1, dim), t, dw)


def sums_kernel(n, mine_ref, dg_ref, dc_ref, loss_ref,
                near, both, chips, total, send_a, recv_a, send_b, recv_b, send_c, recv_c):
    me = lax.axis_index("vp")
    core, chip = lax.rem(me, 2), lax.div(me, 2)
    count = n // 2
    sibling = me + 1 - 2 * core
    dim = dg_ref.shape[1]

    def peer(d):
        return 2 * lax.rem(chip + d, count) + core

    barrier = pltpu.get_barrier_semaphore()
    pl.semaphore_signal(barrier, inc=1, device_id={"vp": sibling}, device_id_type=MESH)
    for d in range(1, count):
        pl.semaphore_signal(barrier, inc=1, device_id={"vp": peer(d)}, device_id_type=MESH)

    pl.semaphore_wait(barrier, count)

    def hop(src, dst, send_sem, recv_sem, who):
        return pltpu.make_async_remote_copy(
            src_ref=src, dst_ref=dst, send_sem=send_sem, recv_sem=recv_sem,
            device_id={"vp": who}, device_id_type=MESH)

    first = hop(mine_ref, near, send_a, recv_a, sibling)
    first.start()
    first.wait_recv()
    both[...] = mine_ref[core] + near[core]

    def second(d):
        return hop(both, chips.at[chip], send_b.at[d], recv_b.at[d], peer(d))

    @pl.loop(1, count)
    def _(d):
        second(d).start()

    chips[chip] = both[...]

    @pl.loop(1, count)
    def _(d):
        second(d).wait()

    total[core] = jnp.sum(chips[...], axis=0)
    third = hop(total.at[core], total.at[core], send_c, recv_c, sibling)
    third.start()
    first.wait_send()
    third.wait()
    dg_ref[...] = total[0, :, 0:dim]
    dc_ref[...] = total[1, :, 0:dim]
    loss_ref[...] = -jnp.sum(total[0, :, dim:], axis=-1, keepdims=True)


def group_sums(n, mine):
    wide = mine.shape[-1]
    dim = wide - 128
    vmem = pl.BlockSpec(memory_space=pltpu.VMEM)
    dma = pltpu.SemaphoreType.DMA
    return pl.pallas_call(
        functools.partial(sums_kernel, n),
        out_shape=(
            jax.ShapeDtypeStruct((1, dim), F32),
            jax.ShapeDtypeStruct((1, dim), F32),
            jax.ShapeDtypeStruct((1, 1), F32),
        ),
        in_specs=[vmem],
        out_specs=(vmem,) * 3,
        scratch_shapes=[
            pltpu.VMEM((2, 1, wide), F32),
            pltpu.VMEM((1, wide), F32),
            pltpu.VMEM((n // 2, 1, wide), F32),
            pltpu.VMEM((2, 1, wide), F32),
            dma, dma, dma((n // 2,)), dma((n // 2,)), dma, dma,
        ],
        compiler_params=pltpu.CompilerParams(collective_id=2, has_side_effects=True, vmem_limit_bytes=16_000_000),
        name="group_sums",
    )(mine)


def solution(mesh):
    n = mesh.shape["vp"]

    def per_device(hidden, norm_gain, norm_bias, w_blk, labels, loss_mask):
        dim = hidden.shape[-1]
        x = hidden.reshape(-1, dim)
        h, z, wt, lse, toks = gather_logits(n, x, norm_gain, norm_bias, labels, loss_mask, w_blk)
        dw, dh, t = scatter_grads(n, z, h, wt, lse, toks)
        grad_x, sums, grad_w = local_backward(dh, x, norm_gain, t, dw)
        grad_gain, grad_bias, loss = group_sums(n, sums)
        return loss.reshape(1), grad_x.reshape(hidden.shape), grad_w, grad_gain.reshape(dim), grad_bias.reshape(dim)

    tok_spec = P("vp", "dp")
    return jax.shard_map(
        per_device,
        mesh=mesh,
        in_specs=(P("vp", "dp", None), P(None), P(None), P(None, "vp"), tok_spec, tok_spec),
        out_specs=(P("dp"), P("vp", "dp", None), P("dp", "vp"), P("dp"), P("dp")),
        check_vma=False,
    )
```

```python
import functools
import math

import jax
import jax.numpy as jnp
from jax import lax
from jax.experimental import pallas as pl
from jax.experimental.pallas import tpu as pltpu
from jax.sharding import PartitionSpec as P

NORM_EPS = 1e-5
MESH = pl.DeviceIdType.MESH
GATHER_VMEM = 62_000_000
F32 = jnp.float32
BF16 = jnp.bfloat16


class Rings:
    def __init__(self, n):
        self.n = n
        self.chips = n // 2
        self.side = math.isqrt(self.chips)
        assert self.side * self.side * 2 == n
        self.me = lax.axis_index("vp")
        self.core = lax.rem(self.me, 2)
        chip = lax.div(self.me, 2)
        x, y = lax.rem(chip, self.side), lax.div(chip, self.side)
        k = lax.rem(x + y, self.side)
        self.spot = (y * self.side + k, x * self.side + k)
        self.sibling = self.me + 1 - 2 * self.core
        step = 2 * self.core - 1
        self.s_next = [self.at(c, lax.rem(self.spot[c] + step + self.chips, self.chips), 1 - self.core) for c in range(2)]
        self.x_prev = [self.at(c, lax.rem(self.spot[c] + step + self.chips, self.chips), 1 - self.core) for c in range(2)]

    def at(self, cycle, spot, core):
        q, k = lax.div(spot, self.side), lax.rem(spot, self.side)
        a = lax.rem(k - q + self.side, self.side)
        chip = q * self.side + a if cycle == 0 else a * self.side + q
        return chip * 2 + core

    def owner(self, group, quarter):
        cycle = quarter % 2
        pos = 2 * self.spot[cycle] + self.core
        shift = self.n - group if quarter < 2 else group
        origin = lax.rem(pos + shift + self.n, self.n)
        return self.at(cycle, lax.div(origin, 2), lax.rem(origin, 2))

    def greet(self):
        barrier = pltpu.get_barrier_semaphore()
        for other in (self.sibling, *self.s_next):
            pl.semaphore_signal(barrier, inc=1, device_id={"vp": other}, device_id_type=MESH)

    def greeted(self):
        pl.semaphore_wait(pltpu.get_barrier_semaphore(), 3)


def norm_rows(x_rows):
    x = x_rows.astype(F32)
    centered = x - jnp.mean(x, axis=-1, keepdims=True)
    inv_std = lax.rsqrt(jnp.mean(centered * centered, axis=-1, keepdims=True) + NORM_EPS)
    return centered * inv_std, inv_std


def signal_all(n, me):
    barrier = pltpu.get_barrier_semaphore()
    for d in range(1, n):
        pl.semaphore_signal(barrier, inc=1, device_id={"vp": lax.rem(me + d, n)}, device_id_type=MESH)


def gather_kernel(n, x_ref, gain_ref, bias_ref, label_ref, mask_ref, w_hbm, h_hbm, z_hbm, wt_hbm, lse_ref, toks_ref,
                  w_v, wt_v, h_all, zbuf, col, local, got, own, tok_ref, w_sem, wt_sem, h_sem, z_sem, send_x, send_s, send_d, recv_x, recv_s,
                  stat_send, stat_recv, lse_send, lse_recv, tok_send, tok_recv):
    ring = Rings(n)
    me = ring.me
    rows, dim = x_ref.shape
    cols = w_v.shape[1]
    half, quart, piece, wide = rows // 2, rows // 4, rows // 8, cols // 2
    xo = pl.multiple_of(half * ring.core, half)
    so = pl.multiple_of(half * (1 - ring.core), half)

    w_copy = pltpu.make_async_copy(w_hbm, w_v, w_sem)
    w_copy.start()
    signal_all(n, me)

    ln_rows = min(64, half)

    def norm_half(base):
        @pl.loop(0, half // ln_rows)
        def _(b):
            r = pl.ds(pl.multiple_of(base + b * ln_rows, ln_rows), ln_rows)
            normed, _ = norm_rows(x_ref[r, :])
            h_all[0, r, :] = (normed * (1.0 + gain_ref[...]) + bias_ref[...]).astype(BF16)

    norm_half(so)
    pl.semaphore_wait(pltpu.get_barrier_semaphore(), n - 1)

    def hop(src, dst, send_sem, recv_sem, who):
        return pltpu.make_async_remote_copy(
            src_ref=src, dst_ref=dst, send_sem=send_sem, recv_sem=recv_sem,
            device_id={"vp": who}, device_id_type=MESH)

    def x_copy(i, c, u):
        r = pl.ds(xo + (c * quart + u * piece), piece)
        return hop(h_all.at[i, r], h_all.at[i + 1, r], send_x.at[lax.rem(i, 4), c, u], recv_s.at[i + 1, c, u], ring.sibling)

    def s_copy(i, c, u):
        r = pl.ds(so + (c * quart + u * piece), piece)
        return hop(h_all.at[i, r], h_all.at[i + 1, r], send_s.at[lax.rem(i, 4), c, u], recv_x.at[i + 1, c, u], ring.s_next[c])

    def d_copy(c, u):
        r = pl.ds(so + (c * quart + u * piece), piece)
        return hop(h_all.at[0, r], h_all.at[n - 1, r], send_d.at[c, u], recv_x.at[n - 1, c, u], ring.sibling)

    for c in range(2):
        s_copy(0, c, 0).start()
    norm_half(xo)

    def x_arrived(i, c, u):
        r = pl.ds(xo + (c * quart + u * piece), piece)
        hop(h_all.at[i, r], h_all.at[i, r], send_s.at[0, c, u], recv_x.at[i, c, u], ring.s_next[c]).wait_recv()

    def s_arrived(i, c, u):
        r = pl.ds(so + (c * quart + u * piece), piece)
        hop(h_all.at[i, r], h_all.at[i, r], send_x.at[0, c, u], recv_s.at[i, c, u], ring.sibling).wait_recv()

    def send(copy, i, c, u):
        @pl.when(i >= 4)
        def _():
            copy(i - 4, c, u).wait_send()
        copy(i, c, u).start()

    def z_out(g, slot):
        return pltpu.make_async_copy(zbuf.at[slot], z_hbm.at[g], z_sem.at[slot])

    def h_out(g, slot):
        return pltpu.make_async_copy(h_all.at[g], h_hbm.at[g], h_sem.at[slot])

    stat_rows = min(32, half)

    def stats(slot, u):
        for b in range(half // stat_rows):
            z = zbuf[slot, u * half + b * stat_rows:u * half + (b + 1) * stat_rows, :]
            top = jnp.max(z, axis=-1, keepdims=True)
            lse = top + jnp.log(jnp.sum(jnp.exp(z - top), axis=-1, keepdims=True))
            col[b * stat_rows:(b + 1) * stat_rows, :] = jnp.broadcast_to(lse, (stat_rows, col.shape[1]))
        return jnp.transpose(col[...])[0:1, :]

    def stat_copy(g, u, c):
        q = 2 * u + c
        return hop(local.at[g, u], got.at[g, q], stat_send, stat_recv, ring.owner(g, q))

    def send_stats(g):
        for u in range(2):
            for c in range(2):
                stat_copy(g, u, c).start()

    def logits(g, slot, u):
        part = slice(u * wide, (u + 1) * wide)
        zbuf[slot, :, part] = jnp.dot(h_all[g], w_v[:, part], preferred_element_type=F32)

    strip = dim // n

    def flip(a, b):
        r = pl.ds(pl.multiple_of(a * (2 * strip), 2 * strip), 2 * strip)
        part = slice(b * wide, (b + 1) * wide)
        wt_v[part, r] = jnp.transpose(w_v[r, part])

    def tok_copy(d):
        return hop(tok_ref, toks_ref.at[me], tok_send, tok_recv, lax.rem(me + d, n))

    def lse_copy(d):
        return hop(own, lse_ref.at[me], lse_send, lse_recv, lax.rem(me + d, n))

    outer, inner = label_ref.shape

    def in_line(block):
        lane = lax.broadcasted_iota(jnp.int32, (inner, rows), 1)
        spread = (lax.rem(lane, inner) == lax.broadcasted_iota(jnp.int32, (inner, rows), 0)).astype(F32)
        line = lax.div(lax.broadcasted_iota(jnp.int32, (outer, rows), 1), inner)
        chosen = line == lax.broadcasted_iota(jnp.int32, (outer, rows), 0)
        return jnp.sum(jnp.where(chosen, jnp.dot(block, spread, preferred_element_type=F32), 0.0), axis=0, keepdims=True)

    def tokens():
        label = label_ref[...]
        high = in_line(lax.shift_right_logical(label, 8).astype(F32))
        tok_ref[:, :rows] = 256.0 * high + in_line((label & 255).astype(F32))
        tok_ref[:, rows:] = in_line(mask_ref[...])

    zbuf[...] = jnp.zeros_like(zbuf)
    w_copy.wait()

    @pl.loop(0, n // 2)
    def _(a):
        for b in range(2):
            i = 2 * a + b
            for u in range(2):
                @pl.when(i >= 1)
                def _():
                    for c in range(2):
                        x_arrived(i, c, u)

                @pl.when(i < n - 1)
                def _():
                    for c in range(2):
                        send(x_copy, i, c, u)

                j = i + u

                @pl.when((j >= 1) & (j < n))
                def _():
                    for c in range(2):
                        s_arrived(j, c, 1 - u)

                @pl.when(j < n - 2)
                def _():
                    for c in range(2):
                        send(s_copy, j, c, 1 - u)

                if u == 0:
                    flip(a, b)
                else:
                    @pl.when(i == 0)
                    def _():
                        for c in range(2):
                            for v in range(2):
                                d_copy(c, v).start()

                        tokens()

                    @pl.when(i == 2)
                    def _():
                        @pl.loop(1, n)
                        def _(d):
                            tok_copy(d).start()

                    @pl.when(i >= 3)
                    def _():
                        send_stats(i - 2)

                if u == 0:
                    @pl.when(i >= 1)
                    def _():
                        logits(i - 1, 1 - b, 1)
                        local[lax.max(i - 2, 0), 1] = stats(b, 1)
                        z_out(i - 1, 1 - b).start()
                else:
                    @pl.when(i >= 2)
                    def _():
                        z_out(i - 2, b).wait()
                        h_out(i - 2, b).wait()
                    h_out(i, b).start()
                    logits(i, b, 0)
                    local[lax.max(i - 1, 0), 0] = stats(1 - b, 0)

    last = n - 1
    wt_copy = pltpu.make_async_copy(wt_v, wt_hbm, wt_sem)
    wt_copy.start()
    logits(last, 1, 1)
    local[last - 1, 1] = stats(0, 1)
    z_out(last, 1).start()
    for u in range(2):
        local[last, u] = stats(1, u)
    send_stats(last - 1)
    send_stats(last)
    for q in range(4):
        got[0, q] = local[0, q // 2]
    toks_ref[me] = tok_ref[...]

    everyone = pl.ds(1, n - 1)
    stats_total = hop(got.at[everyone], got.at[everyone], stat_send, stat_recv, ring.sibling)
    stats_total.wait_recv()
    for q in range(4):
        parts = got[:, q]
        top = jnp.max(parts, axis=0)
        lse = top + jnp.log(jnp.sum(jnp.exp(parts - top[None]), axis=0))
        lanes = slice((q % 2) * quart, (q % 2 + 1) * quart)
        own[:, q * quart:(q + 1) * quart] = lse[:, lanes]
    lse_ref[me] = own[...]

    @pl.loop(1, n)
    def _(d):
        lse_copy(d).start()

    for c in range(2):
        for u in range(2):
            d_copy(c, u).wait_send()
            for i in range(n - 5, n - 1):
                x_copy(i, c, u).wait_send()
            for i in range(n - 6, n - 2):
                s_copy(i, c, u).wait_send()
    stats_total.wait_send()
    toks_total = hop(toks_ref.at[everyone], toks_ref.at[everyone], tok_send, tok_recv, ring.sibling)
    toks_total.wait_recv()
    toks_total.wait_send()
    wt_copy.wait()
    for g in (last - 1, last):
        z_out(g, g % 2).wait()
        h_out(g, g % 2).wait()
    lse_total = hop(lse_ref.at[everyone], lse_ref.at[everyone], lse_send, lse_recv, ring.sibling)
    lse_total.wait_recv()
    lse_total.wait_send()


def gather_logits(n, x, gain, bias, labels, mask, w):
    rows, dim = x.shape
    cols = w.shape[1]
    vmem = pl.BlockSpec(memory_space=pltpu.VMEM)
    hbm = pl.BlockSpec(memory_space=pltpu.HBM)
    dma = pltpu.SemaphoreType.DMA
    return pl.pallas_call(
        functools.partial(gather_kernel, n),
        out_shape=(
            jax.ShapeDtypeStruct((n, rows, dim), BF16),
            jax.ShapeDtypeStruct((n, rows, cols), F32),
            jax.ShapeDtypeStruct((cols, dim), BF16),
            jax.ShapeDtypeStruct((n, 1, rows), F32),
            jax.ShapeDtypeStruct((n, 1, 2 * rows), F32),
        ),
        in_specs=[vmem, vmem, vmem, vmem, vmem, hbm],
        out_specs=(hbm, hbm, hbm, vmem, vmem),
        scratch_shapes=[
            pltpu.VMEM((dim, cols), BF16),
            pltpu.VMEM((cols, dim), BF16),
            pltpu.VMEM((n, rows, dim), BF16),
            pltpu.VMEM((2, rows, cols), F32),
            pltpu.VMEM((rows // 2, 128), F32),
            pltpu.VMEM((n, 2, 1, rows // 2), F32),
            pltpu.VMEM((n, 4, 1, rows // 2), F32),
            pltpu.VMEM((1, rows), F32),
            pltpu.VMEM((1, 2 * rows), F32),
            dma, dma, dma((2,)), dma((2,)), dma((4, 2, 2)), dma((4, 2, 2)), dma((2, 2)), dma((n, 2, 2)), dma((n, 2, 2)),
            dma, dma, dma, dma, dma, dma,
        ],
        compiler_params=pltpu.CompilerParams(collective_id=0, has_side_effects=True, vmem_limit_bytes=GATHER_VMEM),
        name="gather_logits",
    )(x, gain.reshape(1, dim), bias.reshape(1, dim), labels, mask, w)


SLOTS = 8
LAG = 1
PIECES = 4
SCATTER_VMEM = 36_000_000


def scatter_kernel(n, z_hbm, h_hbm, w_hbm, lse_hbm, toks_hbm, dw, dh_ref, t_ref,
                   lse_ref, toks_ref, tok_sem, w_v, zb, hb, dzb, part, from_x, from_s, from_d, flat, cols, w_sem, z_sem, h_sem,
                   send_x, send_s, send_d, recv_x, recv_s, recv_d, credit_x, credit_s):
    ring = Rings(n)
    rows, dim = dh_ref.shape
    vocab = w_v.shape[0]
    half, quart, wide = rows // 2, rows // 4, dim // PIECES
    xo = pl.multiple_of(half * ring.core, half)
    so = pl.multiple_of(half * (1 - ring.core), half)
    col_start = ring.me * vocab

    ring.greet()

    def fetch(hbm, buf, sem, j, slot):
        return [
            pltpu.make_async_copy(
                hbm.at[lax.rem(j + ahead, n), pl.ds(off, half)], buf.at[slot, pl.ds(off, half)], sem.at[slot, ahead])
            for ahead, off in ((0, xo), (1, so))
        ]

    w_copy = pltpu.make_async_copy(w_hbm, w_v, w_sem)
    tok_copies = [pltpu.make_async_copy(lse_hbm, lse_ref, tok_sem.at[0]), pltpu.make_async_copy(toks_hbm, toks_ref, tok_sem.at[1])]
    for copy in tok_copies + fetch(z_hbm, zb, z_sem, 1, 0) + [w_copy] + fetch(h_hbm, hb, h_sem, 1, 0) + fetch(z_hbm, zb, z_sem, 2, 1):
        copy.start()

    flat[...] = jnp.zeros_like(flat)
    dw[...] = jnp.zeros_like(dw)
    for copy in tok_copies:
        copy.wait()
    mask_total = jnp.sum(jnp.sum(toks_ref[:, :, rows:], axis=0), axis=-1, keepdims=True)
    lse_term = jnp.sum(lse_ref[ring.me] * (toks_ref[ring.me][:, rows:] / mask_total), axis=-1, keepdims=True)
    corner = (lax.broadcasted_iota(jnp.int32, t_ref.shape, 0) == 0) & (lax.broadcasted_iota(jnp.int32, t_ref.shape, 1) == 0)
    t_ref[...] = jnp.where(corner, -lse_term, 0.0)

    def columns(j):
        valid = jnp.where(j <= n, 1.0, 0.0)
        for q in range(4):
            group = lax.rem(jnp.where(ring.core == q // 2, j, j + 1), n)
            who = ring.owner(group, q)
            lanes = slice(q * quart, (q + 1) * quart)
            flat[0:1, lanes] = toks_ref[who][:, lanes] - col_start.astype(F32)
            flat[1:2, lanes] = toks_ref[who][:, rows + q * quart:rows + (q + 1) * quart] * valid / mask_total
            flat[2:3, lanes] = lse_ref[who][:, lanes]
        cols[...] = jnp.transpose(flat[...])

    dz_rows = min(16, quart)

    def make_dz(slot, u):
        for b in range(rows // PIECES // dz_rows):
            r = slice(u * (rows // PIECES) + b * dz_rows, u * (rows // PIECES) + (b + 1) * dz_rows)
            z = zb[slot, r, :]
            label = cols[r, 0:1].astype(jnp.int32)
            weight = cols[r, 1:2]
            prob = jnp.exp(z - cols[r, 2:3])
            hit = lax.broadcasted_iota(jnp.int32, z.shape, 1) == label
            dzb[slot, r, :] = (jnp.where(hit, prob - 1.0, prob) * weight).astype(BF16)
            taken = jnp.where(hit, z * weight, 0.0)
            acc = taken[:, 0:128]
            for v in range(1, vocab // 128):
                acc = acc + taken[:, v * 128:(v + 1) * 128]
            t_ref[...] += acc

    def matmuls(now, u, slot):
        dz = dzb[now]
        d = slice(u * wide, (u + 1) * wide)
        part[slot] = jnp.dot(dz, w_v[:, d], preferred_element_type=F32)
        dw[d, :] += lax.dot_general(hb[now, :, d], dz, (((0,), (0,)), ((), ())), preferred_element_type=F32)

    def hop(src, dst, send_sem, recv_sem, who):
        return pltpu.make_async_remote_copy(
            src_ref=src, dst_ref=dst, send_sem=send_sem, recv_sem=recv_sem,
            device_id={"vp": who}, device_id_type=MESH)

    def x_rows(c):
        return pl.ds(xo + c * quart, quart)

    def s_rows(c):
        return pl.ds(so + c * quart, quart)

    def x_copy(slot, c):
        return hop(part.at[slot, x_rows(c)], from_s.at[slot, c], send_x.at[slot, c], recv_s.at[slot, c], ring.sibling)

    def s_copy(slot, c):
        return hop(part.at[slot, s_rows(c)], from_x.at[slot, c], send_s.at[slot, c], recv_x.at[slot, c], ring.s_next[c])

    def d_copy(slot, u, c):
        return hop(part.at[slot, s_rows(c)], from_d.at[u, c], send_d.at[u, c], recv_d.at[u, c], ring.sibling)

    first, end = PIECES, PIECES * n

    def do_x(j, k, slot):
        @pl.when((k >= first + SLOTS) & (k < end))
        def _():
            for c in range(2):
                s_copy(slot, c).wait_recv()
                part[slot, x_rows(c), :] += from_x[slot, c]

        @pl.when((k >= first + SLOTS) & (k < end - PIECES))
        def _():
            for c in range(2):
                pl.semaphore_signal(credit_s.at[c], inc=1, device_id={"vp": ring.s_next[c]}, device_id_type=MESH)

        @pl.when(k < end)
        def _():
            for c in range(2):
                @pl.when(k >= first + SLOTS)
                def _():
                    pl.semaphore_wait(credit_x.at[c], 1)
                x_copy(slot, c).start()

    def do_s(k, slot, u):
        @pl.when((k >= first) & (k < end))
        def _():
            for c in range(2):
                x_copy(slot, c).wait_recv()
                part[slot, s_rows(c), :] += from_s[slot, c]

        @pl.when((k >= first) & (k < end - SLOTS))
        def _():
            for c in range(2):
                pl.semaphore_signal(credit_x.at[c], inc=1, device_id={"vp": ring.sibling}, device_id_type=MESH)

        @pl.when((k >= first) & (k < end - PIECES))
        def _():
            for c in range(2):
                @pl.when(k >= first + SLOTS)
                def _():
                    pl.semaphore_wait(credit_s.at[c], 1)
                s_copy(slot, c).start()

        @pl.when((k >= end - PIECES) & (k < end))
        def _():
            dh_ref[pl.ds(so, half), u * wide:(u + 1) * wide] = part[slot, pl.ds(so, half), :]

    columns(1)
    for copy in fetch(z_hbm, zb, z_sem, 1, 0):
        copy.wait()
    for u in range(PIECES):
        make_dz(0, u)
    for copy in fetch(h_hbm, hb, h_sem, 1, 0):
        copy.wait()
    w_copy.wait()
    ring.greeted()

    @pl.loop(0, n // 2)
    def _(a):
        for b in range(2):
            j = 2 * a + b + 1
            now, then = b, 1 - b

            @pl.when(j < n)
            def _():
                for copy in fetch(z_hbm, zb, z_sem, j + 1, then):
                    copy.wait()
                for copy in fetch(h_hbm, hb, h_sem, j + 1, then):
                    copy.start()

            @pl.when(j < n - 1)
            def _():
                for copy in fetch(z_hbm, zb, z_sem, j + 2, now):
                    copy.start()

            columns(j + 1)
            for u in range(PIECES):
                k = PIECES * j + u
                slot = (PIECES * (b + 1) + u) % SLOTS

                @pl.when(k >= first + SLOTS)
                def _():
                    for c in range(2):
                        x_copy(slot, c).wait_send()
                        s_copy(slot, c).wait_send()

                matmuls(now, u, slot)
                make_dz(then, u)

                @pl.when(j == n)
                def _():
                    for c in range(2):
                        d_copy(slot, u, c).start()

                do_x(j, k, slot)
                do_s(k - LAG, (slot - LAG) % SLOTS, (u - LAG) % PIECES)

            @pl.when(j < n)
            def _():
                for copy in fetch(h_hbm, hb, h_sem, j + 1, then):
                    copy.wait()

    for u in range(PIECES):
        slot = (end + u) % SLOTS
        for c in range(2):
            d_copy(slot, u, c).wait_recv()
            s_copy(slot, c).wait_recv()
            dh_ref[x_rows(c), u * wide:(u + 1) * wide] = part[slot, x_rows(c), :] + from_d[u, c] + from_x[slot, c]
    for u in range(PIECES):
        for c in range(2):
            x_copy((end - PIECES + u) % SLOTS, c).wait_send()
            d_copy((end + u) % SLOTS, u, c).wait_send()


def scatter_grads(n, z, h, w, lse, toks):
    _, rows, vocab = z.shape
    dim = w.shape[1]
    vmem = pl.BlockSpec(memory_space=pltpu.VMEM)
    hbm = pl.BlockSpec(memory_space=pltpu.HBM)
    dma = pltpu.SemaphoreType.DMA
    wide = dim // PIECES
    return pl.pallas_call(
        functools.partial(scatter_kernel, n),
        out_shape=(
            pltpu.VMEM((dim, vocab), F32),
            pltpu.VMEM((rows, dim), F32),
            pltpu.VMEM((16, 128), F32),
        ),
        in_specs=[hbm] * 5,
        out_specs=(vmem, vmem, vmem),
        scratch_shapes=[
            pltpu.VMEM(lse.shape, F32),
            pltpu.VMEM(toks.shape, F32),
            dma((2,)),
            pltpu.VMEM((vocab, dim), BF16),
            pltpu.VMEM((2, rows, vocab), F32),
            pltpu.VMEM((2, rows, dim), BF16),
            pltpu.VMEM((2, rows, vocab), BF16),
            pltpu.VMEM((SLOTS, rows, wide), F32),
            pltpu.VMEM((SLOTS, 2, rows // 4, wide), F32),
            pltpu.VMEM((SLOTS, 2, rows // 4, wide), F32),
            pltpu.VMEM((PIECES, 2, rows // 4, wide), F32),
            pltpu.VMEM((128, rows), F32),
            pltpu.VMEM((rows, 128), F32),
            dma, dma((2, 2)), dma((2, 2)),
            dma((SLOTS, 2)), dma((SLOTS, 2)), dma((PIECES, 2)), dma((SLOTS, 2)), dma((SLOTS, 2)), dma((PIECES, 2)),
            pltpu.SemaphoreType.REGULAR((2,)),
            pltpu.SemaphoreType.REGULAR((2,)),
        ],
        compiler_params=pltpu.CompilerParams(collective_id=1, has_side_effects=True, vmem_limit_bytes=SCATTER_VMEM),
        name="scatter_grads",
    )(z, h, w, pltpu.with_memory_space_constraint(lse, pltpu.HBM), pltpu.with_memory_space_constraint(toks, pltpu.HBM))


DW_COPIES = 8


def local_kernel(dh_ref, x_ref, gain_ref, t_ref, dw_ref, dx_ref, sums_ref, dw_hbm, dw_sem):
    rows, dim = dh_ref.shape
    blk = min(64, rows)
    strip = dw_ref.shape[0] // DW_COPIES
    dw_copies = [
        pltpu.make_async_copy(dw_ref.at[pl.ds(p * strip, strip)], dw_hbm.at[pl.ds(p * strip, strip)], dw_sem.at[p])
        for p in range(DW_COPIES)
    ]
    for copy in dw_copies:
        copy.start()

    def body(b, carry):
        dg, dc = carry
        r = pl.ds(pl.multiple_of(b * blk, blk), blk)
        normed, inv_std = norm_rows(x_ref[r, :])
        dh = dh_ref[r, :]
        dhn = dh * normed
        scaled = dh * (1.0 + gain_ref[...])
        mean_s = jnp.mean(scaled, axis=-1, keepdims=True)
        mean_sn = jnp.mean(scaled * normed, axis=-1, keepdims=True)
        dx_ref[r, :] = (inv_std * (scaled - mean_s - normed * mean_sn)).astype(BF16)
        return dg + jnp.sum(dhn, axis=0, keepdims=True), dc + jnp.sum(dh, axis=0, keepdims=True)

    zero = jnp.zeros((1, dim), F32)
    dg, dc = lax.fori_loop(0, rows // blk, body, (zero, zero))
    sums_ref[0, :, 0:dim] = dg
    sums_ref[1, :, 0:dim] = dc
    sums_ref[0, :, dim:] = jnp.sum(t_ref[...], axis=0, keepdims=True)
    sums_ref[1, :, dim:] = jnp.zeros((1, 128), F32)
    for copy in dw_copies:
        copy.wait()


def local_backward(dh, x, gain, t, dw):
    rows, dim = dh.shape
    vmem = pl.BlockSpec(memory_space=pltpu.VMEM)
    return pl.pallas_call(
        local_kernel,
        out_shape=(
            jax.ShapeDtypeStruct((rows, dim), BF16),
            jax.ShapeDtypeStruct((2, 1, dim + 128), F32),
            jax.ShapeDtypeStruct(dw.shape, F32),
        ),
        in_specs=[vmem] * 5,
        out_specs=(vmem, vmem, pl.BlockSpec(memory_space=pltpu.HBM)),
        scratch_shapes=[pltpu.SemaphoreType.DMA((DW_COPIES,))],
        compiler_params=pltpu.CompilerParams(vmem_limit_bytes=24_000_000),
        name="local_backward",
    )(dh, x, gain.reshape(1, dim), t, dw)


def sums_kernel(n, mine_ref, dg_ref, dc_ref, loss_ref,
                near, both, chips, total, send_a, recv_a, send_b, recv_b, send_c, recv_c):
    me = lax.axis_index("vp")
    core, chip = lax.rem(me, 2), lax.div(me, 2)
    count = n // 2
    sibling = me + 1 - 2 * core
    dim = dg_ref.shape[1]

    def peer(d):
        return 2 * lax.rem(chip + d, count) + core

    barrier = pltpu.get_barrier_semaphore()
    pl.semaphore_signal(barrier, inc=1, device_id={"vp": sibling}, device_id_type=MESH)
    for d in range(1, count):
        pl.semaphore_signal(barrier, inc=1, device_id={"vp": peer(d)}, device_id_type=MESH)

    pl.semaphore_wait(barrier, count)

    def hop(src, dst, send_sem, recv_sem, who):
        return pltpu.make_async_remote_copy(
            src_ref=src, dst_ref=dst, send_sem=send_sem, recv_sem=recv_sem,
            device_id={"vp": who}, device_id_type=MESH)

    first = hop(mine_ref, near, send_a, recv_a, sibling)
    first.start()
    first.wait_recv()
    both[...] = mine_ref[core] + near[core]

    def second(d):
        return hop(both, chips.at[chip], send_b.at[d], recv_b.at[d], peer(d))

    @pl.loop(1, count)
    def _(d):
        second(d).start()

    chips[chip] = both[...]

    @pl.loop(1, count)
    def _(d):
        second(d).wait()

    total[core] = jnp.sum(chips[...], axis=0)
    third = hop(total.at[core], total.at[core], send_c, recv_c, sibling)
    third.start()
    first.wait_send()
    third.wait()
    dg_ref[...] = total[0, :, 0:dim]
    dc_ref[...] = total[1, :, 0:dim]
    loss_ref[...] = -jnp.sum(total[0, :, dim:], axis=-1, keepdims=True)


def group_sums(n, mine):
    wide = mine.shape[-1]
    dim = wide - 128
    vmem = pl.BlockSpec(memory_space=pltpu.VMEM)
    dma = pltpu.SemaphoreType.DMA
    return pl.pallas_call(
        functools.partial(sums_kernel, n),
        out_shape=(
            jax.ShapeDtypeStruct((1, dim), F32),
            jax.ShapeDtypeStruct((1, dim), F32),
            jax.ShapeDtypeStruct((1, 1), F32),
        ),
        in_specs=[vmem],
        out_specs=(vmem,) * 3,
        scratch_shapes=[
            pltpu.VMEM((2, 1, wide), F32),
            pltpu.VMEM((1, wide), F32),
            pltpu.VMEM((n // 2, 1, wide), F32),
            pltpu.VMEM((2, 1, wide), F32),
            dma, dma, dma((n // 2,)), dma((n // 2,)), dma, dma,
        ],
        compiler_params=pltpu.CompilerParams(collective_id=2, has_side_effects=True, vmem_limit_bytes=16_000_000),
        name="group_sums",
    )(mine)


def solution(mesh):
    n = mesh.shape["vp"]

    def per_device(hidden, norm_gain, norm_bias, w_blk, labels, loss_mask):
        dim = hidden.shape[-1]
        x = hidden.reshape(-1, dim)
        h, z, wt, lse, toks = gather_logits(n, x, norm_gain, norm_bias, labels, loss_mask, w_blk)
        dw, dh, t = scatter_grads(n, z, h, wt, lse, toks)
        grad_x, sums, grad_w = local_backward(dh, x, norm_gain, t, dw)
        grad_gain, grad_bias, loss = group_sums(n, sums)
        return loss.reshape(1), grad_x.reshape(hidden.shape), grad_w, grad_gain.reshape(dim), grad_bias.reshape(dim)

    tok_spec = P("vp", "dp")
    return jax.shard_map(
        per_device,
        mesh=mesh,
        in_specs=(P("vp", "dp", None), P(None), P(None), P(None, "vp"), tok_spec, tok_spec),
        out_specs=(P("dp"), P("vp", "dp", None), P("dp", "vp"), P("dp"), P("dp")),
        check_vma=False,
    )
```
